128 devices in a mesh: gx: 4 (over x), gy: 32 (over z, y, core).
Axes of the slice: x: 4, y: 4, z: 4, core: 2. Of those that a mesh axis runs over, the one named last changes fastest.
Arguments:
- schur_blocks: float32 [128, 2048, 2048], P(('gx', 'gy')), may hold values from -1 to 11, as said below
- offsets: int32 [128], P(('gx', 'gy')), may hold values from 256 to 768, as said below
- right_side: float32 [131072, 128], P(('gx', 'gy')), may hold values from -20 to 20
- coarse_basis: float32 [131072, 128], P(('gx', 'gy')), may hold values from -0.015625 to 0.015625
- coarse_load: float32 [128, 128], replicated, may hold values from -6 to 6
Outputs:
- multipliers: float32 [131072, 128], P(('gx', 'gy'))
- amplitudes: float32 [128, 128], replicated
The draws below stay inside these ranges and needn't reach their ends.
Inputs may be any that keep to these rules, and one draw needn't show every extreme that they name: `schur_blocks`: each block is symmetric positive definite. `offsets`: both ends of the range are taken by some subdomain.
All inputs are finite; a program needn't handle non-finite values.
Results may differ from the reference program's by a relative error of at most 0.0003.
Values sent between devices are 32-bit elements; how exact they have to be, the bound alone decides.
No kernel may reach another device: no remote copies, remote signals or barrier semaphores. Data moves between devices by JAX's collectives and lax.ppermute only.
A program may use at most 128 MiB of HBM per device.

```python
import math
import jax
import jax.numpy as jnp
from jax import lax

W = 2048
SLAB = 1024
R = 128
NC = 128
ITERS = 3
SUBDOMAINS = 128
MULTS = 131072


def draw_schur_blocks(key, part):
    upper_end = 4.0
    subkeys = jax.random.split(key, SUBDOMAINS)

    def single(subkey):
        diag_key, noise_key = jax.random.split(subkey)
        diagonal = jnp.exp(jax.random.uniform(diag_key, (W,), jnp.float32, 0.0, math.log(upper_end)))
        noise_part = jax.random.truncated_normal(noise_key, -5.0, 5.0, (W, W), jnp.float32) * (0.25 / math.sqrt(W))
        return jnp.diag(diagonal) + (noise_part + noise_part.T) * 0.7071067811865476
    return lax.map(single, subkeys)


def draw_offsets(key, part):
    key_values, key_ranking = jax.random.split(key)
    lowest = SLAB // 4
    highest = 3 * SLAB // 4
    values = jax.random.randint(key_values, (SUBDOMAINS,), lowest, highest + 1).astype(jnp.int32)
    ranking = jax.random.permutation(key_ranking, SUBDOMAINS)
    values = values.at[ranking[0]].set(lowest).at[ranking[1]].set(highest)
    return values.astype(jnp.int32)


def draw_right_side(key, part):
    base_key = jax.random.fold_in(key, 0)
    total_rows = SLAB * SUBDOMAINS
    position = jnp.arange(total_rows, dtype=jnp.float32) / total_rows
    base = jax.random.truncated_normal(base_key, -4.0, 4.0, (total_rows, R), jnp.float32)
    rising = 1.0 + 2.0 * position
    return base * rising[:, None]


def block_scale(stream_key, dims, cuts, low, top_value):
    gain, own = 1.0, jax.random.fold_in(stream_key, 6)
    for dim, shards_of in cuts:
        heights = jnp.exp(jax.random.uniform(jax.random.fold_in(own, dim), (shards_of,), jnp.float32, low / len(cuts), top_value / len(cuts)))
        gain = gain * jnp.repeat(heights, dims[dim] // shards_of).reshape([-1 if axis == dim else 1 for axis in range(len(dims))])
    return gain


def gaussian(stream_key, extent, spread, reach, pieces=(), kind=jnp.bfloat16):
    values = jax.random.normal(stream_key, extent, jnp.float32) * spread
    if len(pieces) > 0:
        values = block_scale(stream_key, extent, pieces, -0.22, 0.18) * values
    return jnp.clip(values, min=-reach, max=reach).astype(kind)


def setup_inputs(seed: int = 0) -> dict:
    keys = jax.random.split(jax.random.key(seed), 6)
    return {
        "schur_blocks": draw_schur_blocks(jax.random.fold_in(keys[5], 71), 0),
        "offsets": draw_offsets(jax.random.fold_in(keys[5], 71), 0),
        "right_side": draw_right_side(jax.random.fold_in(keys[5], 71), 0),
        "coarse_basis": gaussian(keys[3], (MULTS, NC), MULTS ** -0.5, 0.015625, ((0, 128),), jnp.float32),
        "coarse_load": gaussian(keys[4], (NC, R), 1.0, 6.0, (), jnp.float32),
    }


HIGHEST = lax.Precision.HIGHEST

def apply_operator(vector, schur_blocks, offsets):
    padded = jnp.pad(vector, ((SLAB, SLAB), (0, 0)))

    def visit_block(accumulated, inputs):
        schur_block, start_row, device_index = inputs
        first_row = (device_index * SLAB + start_row).astype(jnp.int32)
        window = lax.dynamic_slice_in_dim(padded, first_row, W, 0)
        product_block = jnp.dot(schur_block.astype(jnp.float32), window.astype(jnp.float32), precision=HIGHEST, preferred_element_type=jnp.float32)
        current = lax.dynamic_slice_in_dim(accumulated, first_row, W, 0)
        return (lax.dynamic_update_slice_in_dim(accumulated, current + product_block, first_row, 0), None)
    indices = jnp.arange(SUBDOMAINS, dtype=jnp.int32)
    accumulated, _ = lax.scan(visit_block, jnp.zeros_like(padded), (schur_blocks, offsets.astype(jnp.int32), indices))
    return accumulated[SLAB:SLAB + vector.shape[0]]

def project(residual, coarse_basis, gram_factor):
    coarse_part = jnp.dot(coarse_basis.T.astype(jnp.float32), residual.astype(jnp.float32), precision=HIGHEST, preferred_element_type=jnp.float32)
    amplitudes = jax.scipy.linalg.cho_solve((gram_factor, True), coarse_part)
    projected = residual - jnp.dot(coarse_basis.astype(jnp.float32), amplitudes.astype(jnp.float32), precision=HIGHEST, preferred_element_type=jnp.float32)
    return (projected, amplitudes)

def reference(schur_blocks, offsets, right_side, coarse_basis, coarse_load):
    gram_matrix = jnp.dot(coarse_basis.T.astype(jnp.float32), coarse_basis.astype(jnp.float32), precision=HIGHEST, preferred_element_type=jnp.float32)
    gram_factor = jnp.linalg.cholesky(gram_matrix)
    start_load = jax.scipy.linalg.cho_solve((gram_factor, True), coarse_load)
    multipliers = jnp.dot(coarse_basis.astype(jnp.float32), start_load.astype(jnp.float32), precision=HIGHEST, preferred_element_type=jnp.float32)
    residual = right_side - apply_operator(multipliers, schur_blocks, offsets)
    projected, amplitudes = project(residual, coarse_basis, gram_factor)
    direction = projected
    energy_now = jnp.sum(projected * projected, axis=0)
    for iteration in range(ITERS):
        operator_image = apply_operator(direction, schur_blocks, offsets)
        step_length = energy_now / jnp.sum(direction * operator_image, axis=0)
        multipliers = multipliers + step_length * direction
        residual = residual - step_length * operator_image
        projected, amplitudes = project(residual, coarse_basis, gram_factor)
        energy_next = jnp.sum(projected * projected, axis=0)
        direction = projected + energy_next / energy_now * direction
        energy_now = energy_next
    return (multipliers, amplitudes)
```

```python
import jax
import jax.numpy as jnp
from jax import lax
from jax.experimental import pallas as pl
from jax.experimental.pallas import tpu as pltpu
from jax.sharding import Mesh
from jax.sharding import PartitionSpec as P

GX_GY = ("gx", "gy_0", "gy_1", "gy_2")
HIGHEST = lax.Precision.HIGHEST
F32 = jnp.float32
BF16 = jnp.bfloat16

SLAB = 1024
WINDOW = 2048
REACH = 768
SKIP = SLAB - REACH
EXT = SLAB + 2 * REACH
R = 128
DEVICES = 128
TILE = 256


def full_dot(a, b):
    return jnp.dot(a, b, precision=HIGHEST, preferred_element_type=F32)


def contract_rows(a, b):
    return lax.dot_general(
        a, b, (((0,), (0,)), ((), ())), precision=HIGHEST, preferred_element_type=F32
    )


def split_bf16(x):
    high = x.astype(BF16)
    return high, (x - high.astype(F32)).astype(BF16)


def operator_kernel(start_ref, ext_ref, left_ref, schur_ref, *refs, spread):
    if spread:
        low_ref, own_ref, up_ref, energy_ref, cross_ref, halves, image = refs
    else:
        energy_ref, halves = refs
    step = pl.program_id(0)
    start = start_ref[0] - SKIP

    @pl.when(step == 0)
    def _():
        high, low = split_bf16(ext_ref[pl.ds(start, WINDOW), :])
        halves[:, :R] = high
        halves[:, R:] = low
        energy_ref[...] = jnp.zeros_like(energy_ref)
        if spread:
            cross_ref[...] = jnp.zeros_like(cross_ref)
            image[: EXT - WINDOW, :] = jnp.zeros((EXT - WINDOW, R), F32)
            image[WINDOW:, :] = jnp.zeros((EXT - WINDOW, R), F32)

    high, low = split_bf16(schur_ref[...])
    both = jnp.dot(high, halves[...], preferred_element_type=F32)
    rest = jnp.dot(low, halves[:, :R], preferred_element_type=F32)
    product = both[:, :R] + both[:, R:] + rest
    rows = pl.ds(start + step * TILE, TILE)
    energy_ref[...] += jnp.sum((ext_ref[rows, :] * product).reshape(TILE // 8, 8, R), axis=0)
    if spread:
        cross_ref[...] += contract_rows(left_ref[rows, :], product)
        image[rows, :] = product

        @pl.when(step == pl.num_programs(0) - 1)
        def _():
            low_ref[...] = image[:REACH, :]
            own_ref[...] = image[REACH : REACH + SLAB, :]
            up_ref[...] = image[REACH + SLAB :, :]


def apply_operator(start, ext, left, schur, spread=True):
    whole = lambda rows: pl.BlockSpec((rows, R), lambda i: (0, 0))
    shapes = [jax.ShapeDtypeStruct((8, R), F32)]
    out_specs = [whole(8)]
    scratch = [pltpu.VMEM((WINDOW, 2 * R), BF16)]
    if spread:
        rows = (REACH, SLAB, REACH)
        shapes = [jax.ShapeDtypeStruct((n, R), F32) for n in rows] + shapes
        shapes += [jax.ShapeDtypeStruct((R, R), F32)]
        out_specs = [whole(n) for n in rows] + out_specs + [whole(R)]
        scratch += [pltpu.VMEM((EXT, R), F32)]
    out = pl.pallas_call(
        lambda *refs: operator_kernel(*refs, spread=spread),
        grid=(WINDOW // TILE,),
        in_specs=[
            pl.BlockSpec(memory_space=pltpu.SMEM),
            whole(EXT),
            whole(EXT),
            pl.BlockSpec((None, TILE, WINDOW), lambda i: (0, i, 0)),
        ],
        out_specs=out_specs,
        out_shape=shapes,
        scratch_shapes=scratch,
        compiler_params=pltpu.CompilerParams(
            dimension_semantics=("arbitrary",), vmem_limit_bytes=32 << 20
        ),
        cost_estimate=pl.CostEstimate(
            flops=6 * WINDOW * WINDOW * R, bytes_accessed=4 * WINDOW * WINDOW, transcendentals=0
        ),
        name="operator",
    )(start, ext, left, schur)
    if spread:
        low, own, up, energy, cross = out
        return (low, own, up), jnp.sum(energy, axis=0), cross
    return jnp.sum(out[0], axis=0)


def inverse_kernel(gram_ref, inverse_ref):
    gram = gram_ref[...]
    row = lax.broadcasted_iota(jnp.int32, (R, R), 0)
    column = lax.broadcasted_iota(jnp.int32, (R, R), 1)
    identity = jnp.where(row == column, 1.0, 0.0).astype(F32)
    diagonal = gram * identity
    across = lax.rsqrt(jnp.sum(diagonal, axis=0, keepdims=True))
    along = lax.rsqrt(jnp.sum(diagonal, axis=1, keepdims=True))
    scaled = gram * across * along
    bound = jnp.max(jnp.sum(jnp.abs(scaled), axis=0, keepdims=True), axis=1, keepdims=True)
    inverse_ref[...] = identity / bound

    def refine():
        current = inverse_ref[...]
        rest = identity - full_dot(scaled, current)
        inverse_ref[...] = current + full_dot(current, rest)
        return jnp.max(jnp.abs(rest))

    def body(carry):
        return carry[0] + 1, refine()

    lax.while_loop(lambda c: (c[0] < 60) & (c[1] > 1e-3), body, (jnp.int32(0), jnp.float32(1.0)))
    refine()
    inverse_ref[...] = inverse_ref[...] * across * along


def inverse_of(gram):
    return pl.pallas_call(
        inverse_kernel,
        out_shape=jax.ShapeDtypeStruct((R, R), F32),
        in_specs=[pl.BlockSpec(memory_space=pltpu.VMEM)],
        out_specs=pl.BlockSpec(memory_space=pltpu.VMEM),
        compiler_params=pltpu.CompilerParams(vmem_limit_bytes=4 << 20),
        cost_estimate=pl.CostEstimate(flops=400 * R * R * R, bytes_accessed=8 * R * R, transcendentals=0),
        name="inverse",
    )(gram)


UP = [(i, i + 1) for i in range(DEVICES - 1)]
DOWN = [(i + 1, i) for i in range(DEVICES - 1)]


def extended(own):
    low = lax.ppermute(own[SKIP:], GX_GY, UP)
    high = lax.ppermute(own[:REACH], GX_GY, DOWN)
    return jnp.concatenate([low, own, high], axis=0)


def gathered_sum(parts):
    to_low, own, to_high = parts
    from_high = lax.ppermute(to_low, GX_GY, DOWN)
    from_low = lax.ppermute(to_high, GX_GY, UP)
    return own + jnp.pad(from_low, ((0, SKIP), (0, 0))) + jnp.pad(from_high, ((SKIP, 0), (0, 0)))


def exchange(*pieces):
    pieces = [jnp.broadcast_to(p, (DEVICES, p.shape[-1])) for p in pieces]
    joined = jnp.concatenate(pieces, axis=1)
    width = joined.shape[1]
    arrived = lax.all_to_all(joined.reshape(DEVICES, 1, width), GX_GY, 0, 0, tiled=True)
    return arrived.reshape(DEVICES, width)


def columns(array, *indices):
    return [array[:, R * i : R * (i + 1)] for i in indices]


def sums(array, *indices):
    return [jnp.sum(array[:, R * i : R * (i + 1)], axis=0, keepdims=True) for i in indices]


def column_sum(a, b):
    return jnp.sum(a * b, axis=0, keepdims=True)


def local(schur, offsets, right_side, basis, load):
    start = offsets

    basis_ext = extended(basis)
    parts, _, stiff = apply_operator(start, basis_ext, basis_ext, schur)
    arrived = exchange(contract_rows(basis, basis), contract_rows(basis, right_side), stiff)
    mine = sums(arrived, 0, 1, 2)
    image = gathered_sum(parts)
    image_ext = extended(image)
    right_ext = extended(right_side)
    arrived = exchange(*mine, contract_rows(image, image))
    gram, coarse, stiff = columns(arrived, 0, 1, 2)
    (mine_square,) = sums(arrived, 3)
    inverse = inverse_of(gram)
    first = full_dot(inverse, load)
    amp = full_dot(inverse, coarse - full_dot(stiff, first))
    r0_ext = right_ext - full_dot(image_ext, first) - full_dot(basis_ext, amp)
    r0 = r0_ext[REACH : REACH + SLAB]

    parts, form, cross = apply_operator(start, r0_ext, image_ext, schur)
    arrived = exchange(column_sum(r0, r0), form[None], mine_square, contract_rows(image, r0), cross)
    w0 = gathered_sum(parts)
    w0_ext = extended(w0)
    energy0, form0 = sums(arrived, 0, 1)
    (square,) = columns(arrived, 2)
    mine = sums(arrived, 3, 4)
    step0 = energy0 / form0
    r1_ext = r0_ext - step0 * w0_ext
    r1 = r1_ext[REACH : REACH + SLAB]

    parts, form, cross = apply_operator(start, r1_ext, image_ext, schur)
    arrived = exchange(column_sum(r1, r1), form[None], *mine, cross)
    w1 = gathered_sum(parts)
    w1_ext = extended(w1)
    norm1, form1 = sums(arrived, 0, 1)
    e0, f0 = columns(arrived, 2, 3)
    mine = sums(arrived, 4)
    c1 = -step0 * e0
    a1 = full_dot(inverse, c1)
    e1 = e0 - step0 * f0
    energy1 = norm1 - column_sum(c1, a1)
    stiff_a1 = full_dot(stiff, a1)
    ratio0 = energy1 / energy0
    curve1 = form1 - 2.0 * column_sum(a1, e1) + column_sum(a1, stiff_a1) - ratio0 * energy1 / step0
    step1 = energy1 / curve1
    d1_image = w1_ext - full_dot(image_ext, a1) + ratio0 * w0_ext
    r2_ext = r1_ext - step1 * d1_image
    r2 = r2_ext[REACH : REACH + SLAB]
    d1 = r1 - full_dot(basis, a1) + ratio0 * r0
    d1_coarse = e1 - stiff_a1 + ratio0 * e0
    c2 = c1 - step1 * d1_coarse
    a2 = full_dot(inverse, c2)
    square_a1 = full_dot(square, a1)

    form = apply_operator(start, r2_ext, image_ext, schur, spread=False)
    arrived = exchange(column_sum(r2, r2), form[None], *mine)
    norm2, form2 = sums(arrived, 0, 1)
    (f1,) = columns(arrived, 2)
    e2 = e1 - step1 * (f1 - square_a1 + ratio0 * f0)
    energy2 = norm2 - column_sum(c2, a2)
    stiff_a2 = full_dot(stiff, a2)
    ratio1 = energy2 / energy1
    curve2 = form2 - 2.0 * column_sum(a2, e2) + column_sum(a2, stiff_a2) - ratio1 * energy2 / step1
    step2 = energy2 / curve2
    d2 = r2 - full_dot(basis, a2) + ratio1 * d1
    c3 = c2 - step2 * (e2 - stiff_a2 + ratio1 * d1_coarse)
    multipliers = full_dot(basis, first) + step0 * r0 + step1 * d1 + step2 * d2
    return multipliers, amp + full_dot(inverse, c3)


def solution(mesh):
    split = Mesh(mesh.devices.reshape(mesh.shape["gx"], 4, 4, 2), GX_GY)
    in_specs = (P(GX_GY, None, None), P(GX_GY), P(GX_GY, None), P(GX_GY, None), P())
    out_specs = (P(GX_GY, None), P())
    return jax.shard_map(local, mesh=split, in_specs=in_specs, out_specs=out_specs, check_vma=False)
```

```python
import functools

import jax
import jax.numpy as jnp
from jax import lax
from jax.experimental import pallas as pl
from jax.experimental.pallas import tpu as pltpu
from jax.sharding import Mesh
from jax.sharding import PartitionSpec as P

GX_GY = ("gx", "gy_0", "gy_1", "gy_2")
HIGHEST = lax.Precision.HIGHEST
F32 = jnp.float32
BF16 = jnp.bfloat16

SLAB = 1024
WINDOW = 2048
REACH = 768
SKIP = SLAB - REACH
HIGH = REACH + SLAB
EXT = SLAB + 2 * REACH
R = 128
DEVICES = 128
TILE = 256
STEPS = WINDOW // TILE
OWN = slice(REACH, HIGH)

MATRIX = jax.ShapeDtypeStruct((R, R), F32)
EXTENDED = jax.ShapeDtypeStruct((EXT, R), F32)


def full_dot(a, b):
    return jnp.dot(a, b, precision=HIGHEST, preferred_element_type=F32)


def contract_rows(a, b):
    return lax.dot_general(
        a, b, (((0,), (0,)), ((), ())), precision=HIGHEST, preferred_element_type=F32
    )


def split_bf16(x):
    high = x.astype(BF16)
    return high, (x - high.astype(F32)).astype(BF16)


def column_sum(a, b):
    return jnp.sum(a * b, axis=0, keepdims=True)


def part(arrived, index, count):
    return arrived[pl.ds(index, DEVICES, stride=count), :]


def total(arrived, index, count):
    return jnp.sum(part(arrived, index, count), axis=0, keepdims=True)


def put(joined, index, count, value):
    joined[pl.ds(index, DEVICES, stride=count), :] = jnp.broadcast_to(value, (DEVICES, R))


def sides(parity, scale):
    partner = pl.multiple_of(scale * (1 - parity), 8)
    remote = pl.multiple_of(scale * parity, 8)
    return pl.ds(partner, REACH), pl.ds(remote, REACH)


def assemble(ext, pieces, parity):
    own, partner, remote = pieces
    at_partner, at_remote = sides(parity, HIGH)
    ext[OWN, :] = own[...]
    ext[at_partner, :] = partner[...]
    ext[at_remote, :] = remote[...]


def invert(gram, inverse):
    row = lax.broadcasted_iota(jnp.int32, (R, R), 0)
    column = lax.broadcasted_iota(jnp.int32, (R, R), 1)
    identity = jnp.where(row == column, 1.0, 0.0).astype(F32)
    diagonal = gram * identity
    across = lax.rsqrt(jnp.sum(diagonal, axis=0, keepdims=True))
    along = lax.rsqrt(jnp.sum(diagonal, axis=1, keepdims=True))
    scaled = gram * across * along
    bound = jnp.max(jnp.sum(jnp.abs(scaled), axis=0, keepdims=True), axis=1, keepdims=True)
    inverse[...] = identity / bound

    def refine():
        current = inverse[...]
        rest = identity - full_dot(scaled, current)
        inverse[...] = current + full_dot(current, rest)
        return jnp.max(jnp.abs(rest))

    def body(carry):
        return carry[0] + 1, refine()

    lax.while_loop(lambda c: (c[0] < 60) & (c[1] > 1e-3), body, (jnp.int32(0), jnp.float32(1.0)))
    refine()
    inverse[...] = inverse[...] * across * along


def multiply(start, step, ext, schur, halves):
    @pl.when(step == 0)
    def _():
        high, low = split_bf16(ext[pl.ds(start, WINDOW), :])
        halves[:, :R] = high
        halves[:, R:] = low

    high, low = split_bf16(schur[...])
    both = jnp.dot(high, halves[...], preferred_element_type=F32)
    rest = jnp.dot(low, halves[:, :R], preferred_element_type=F32)
    return both[:, :R] + both[:, R:] + rest


def add_form(form, ext, rows, product):
    form[...] += jnp.sum((ext[rows, :] * product).reshape(TILE // 8, 8, R), axis=0)


def clear(form, cross, image):
    form[...] = jnp.zeros_like(form)
    cross[...] = jnp.zeros_like(cross)
    image[: EXT - WINDOW, :] = jnp.zeros((EXT - WINDOW, R), F32)
    image[WINDOW:, :] = jnp.zeros((EXT - WINDOW, R), F32)


def deliver(image, parity, own, partner, remote):
    at_partner, at_remote = sides(parity, HIGH)
    own[...] = image[OWN, :]
    partner[...] = image[at_partner, :]
    remote[...] = image[at_remote, :]


def first_kernel(
    place, own, partner, remote, gram, coarse, schur,
    out_own, out_partner, out_remote, joined,
    ext, halves, image, form, cross,
):
    step = pl.program_id(0)
    start, parity = place[0] - SKIP, place[1]

    @pl.when(step == 0)
    def _():
        assemble(ext, (own, partner, remote), parity)
        clear(form, cross, image)
        put(joined, 0, 3, gram[...])
        put(joined, 1, 3, coarse[...])

    product = multiply(start, step, ext, schur, halves)
    rows = pl.ds(start + step * TILE, TILE)
    cross[...] += contract_rows(ext[rows, :], product)
    image[rows, :] = product

    @pl.when(step == STEPS - 1)
    def _():
        deliver(image, parity, out_own, out_partner, out_remote)
        put(joined, 2, 3, cross[...])


def start_kernel(
    place, arrived, load, square,
    right_own, right_partner, right_remote,
    basis_own, basis_partner, basis_remote,
    image_own, image_partner, image_remote, schur,
    out_own, out_partner, out_remote, joined,
    residual, z_ext, inverse, first, amp, stiff,
    halves, image, form, cross, early,
):
    step = pl.program_id(0)
    start, parity = place[0] - SKIP, place[1]

    @pl.when(step == 0)
    def _():
        invert(part(arrived, 0, 3), inverse)
        stiff[...] = part(arrived, 2, 3)
        first[...] = full_dot(inverse[...], load[...])
        amp[...] = full_dot(inverse[...], part(arrived, 1, 3) - full_dot(stiff[...], first[...]))
        assemble(z_ext, (image_own, image_partner, image_remote), parity)
        assemble(image, (basis_own, basis_partner, basis_remote), parity)
        assemble(residual, (right_own, right_partner, right_remote), parity)
        residual[...] = (
            residual[...]
            - full_dot(z_ext[...], first[...])
            - full_dot(image[...], amp[...])
        )
        clear(form, cross, image)
        own = residual[OWN, :]
        put(joined, 0, 5, column_sum(own, own))
        put(joined, 4, 5, square[...])
        early[...] = contract_rows(image_own[...], own)
        put(joined, 2, 5, early[...])

    product = multiply(start, step, residual, schur, halves)
    rows = pl.ds(start + step * TILE, TILE)
    add_form(form, residual, rows, product)
    cross[...] += contract_rows(z_ext[rows, :], product)
    image[rows, :] = product

    @pl.when(step == STEPS - 1)
    def _():
        deliver(image, parity, out_own, out_partner, out_remote)
        put(joined, 1, 5, jnp.sum(form[...], axis=0, keepdims=True))
        put(joined, 3, 5, cross[...])


def middle_kernel(
    place, arrived, last, z_ext, own, partner, remote, schur,
    out_own, out_partner, out_remote, joined, residual, w_ext, scalars,
    halves, image, form, cross,
):
    step = pl.program_id(0)
    start, parity = place[0] - SKIP, place[1]

    @pl.when(step == 0)
    def _():
        energy = total(arrived, 0, 5)
        length = energy / total(arrived, 1, 5)
        assemble(w_ext, (own, partner, remote), parity)
        residual[...] = last[...] - length * w_ext[...]
        clear(form, cross, image)
        mine = residual[OWN, :]
        put(joined, 0, 5, column_sum(mine, mine))
        put(joined, 2, 5, total(arrived, 2, 5))
        put(joined, 3, 5, total(arrived, 3, 5))
        scalars[...] = jnp.zeros_like(scalars)
        scalars[0:1, :] = energy
        scalars[1:2, :] = length
        scalars[2:3, :] = total(arrived, 4, 5)

    product = multiply(start, step, residual, schur, halves)
    rows = pl.ds(start + step * TILE, TILE)
    add_form(form, residual, rows, product)
    cross[...] += contract_rows(z_ext[rows, :], product)
    image[rows, :] = product

    @pl.when(step == STEPS - 1)
    def _():
        deliver(image, parity, out_own, out_partner, out_remote)
        put(joined, 1, 5, jnp.sum(form[...], axis=0, keepdims=True))
        put(joined, 4, 5, cross[...])


def last_kernel(
    place, arrived, scalars, last, w_last, z_ext, own, partner, remote, inverse, stiff, schur,
    joined, new_own, numbers, matrices,
    residual, halves, form, w_ext,
):
    step = pl.program_id(0)
    start, parity = place[0] - SKIP, place[1]

    @pl.when(step == 0)
    def _():
        energy0, length0 = scalars[0:1, :], scalars[1:2, :]
        e0, f0 = part(arrived, 2, 5), part(arrived, 3, 5)
        c1 = -length0 * e0
        a1 = full_dot(inverse[...], c1)
        e1 = e0 - length0 * f0
        energy1 = total(arrived, 0, 5) - column_sum(c1, a1)
        stiff_a1 = full_dot(stiff[...], a1)
        ratio0 = energy1 / energy0
        curve1 = (
            total(arrived, 1, 5)
            - 2.0 * column_sum(a1, e1)
            + column_sum(a1, stiff_a1)
            - ratio0 * energy1 / length0
        )
        length1 = energy1 / curve1
        assemble(w_ext, (own, partner, remote), parity)
        residual[...] = last[...] - length1 * (
            w_ext[...] - full_dot(z_ext[...], a1) + ratio0 * w_last[...]
        )
        mine = residual[OWN, :]
        new_own[...] = mine
        put(joined, 0, 4, column_sum(mine, mine))
        put(joined, 2, 4, total(arrived, 4, 5))
        put(joined, 3, 4, scalars[2:3, :])
        numbers[...] = jnp.zeros_like(numbers)
        numbers[0:1, :] = length0
        numbers[1:2, :] = length1
        numbers[2:3, :] = ratio0
        numbers[3:4, :] = energy1
        d_coarse = e1 - stiff_a1 + ratio0 * e0
        matrices[0] = a1
        matrices[1] = c1 - length1 * d_coarse
        matrices[2] = d_coarse
        matrices[3] = e1 - length1 * ratio0 * f0
        form[...] = jnp.zeros_like(form)

    product = multiply(start, step, residual, schur, halves)
    add_form(form, residual, pl.ds(start + step * TILE, TILE), product)

    @pl.when(step == STEPS - 1)
    def _():
        put(joined, 1, 4, jnp.sum(form[...], axis=0, keepdims=True))


def direction_kernel(
    numbers, matrices, inverse, stiff, first, basis, r0, r1, r2,
    base, d1, p2, small,
):
    length0, length1, ratio0 = numbers[0:1, :], numbers[1:2, :], numbers[2:3, :]
    a1 = matrices[0]
    a2 = full_dot(inverse[...], matrices[1])
    d1[...] = r1[...] - full_dot(basis[...], a1) + ratio0 * r0[...]
    p2[...] = r2[...] - full_dot(basis[...], a2)
    base[...] = full_dot(basis[...], first[...]) + length0 * r0[...] + length1 * d1[...]
    small[0] = a2
    small[1] = full_dot(stiff[...], a2)


def final_kernel(
    arrived, numbers, matrices, small, inverse, amp, base, d1, p2,
    multipliers, amplitudes,
):
    length1, energy1 = numbers[1:2, :], numbers[3:4, :]
    a2, stiff_a2 = small[0], small[1]
    f1, square = part(arrived, 2, 4), part(arrived, 3, 4)
    e2 = matrices[3] - length1 * (f1 - full_dot(square, matrices[0]))
    energy2 = total(arrived, 0, 4) - column_sum(matrices[1], a2)
    ratio1 = energy2 / energy1
    curve2 = (
        total(arrived, 1, 4)
        - 2.0 * column_sum(a2, e2)
        + column_sum(a2, stiff_a2)
        - ratio1 * energy2 / length1
    )
    length2 = energy2 / curve2
    multipliers[...] = base[...] + length2 * (p2[...] + ratio1 * d1[...])
    c3 = matrices[1] - length2 * (e2 - stiff_a2 + ratio1 * matrices[2])
    amplitudes[...] = amp[...] + full_dot(inverse[...], c3)


def sum_kernel(place, own, partner, remote, total_own, to_partner, to_remote):
    at_partner, at_remote = sides(place[1], SKIP)
    total_own[...] = own[...]
    total_own[at_partner, :] += partner[...]
    total_own[at_remote, :] += remote[...]
    to_partner[...] = total_own[at_partner, :]
    to_remote[...] = total_own[at_remote, :]


def turn_kernel(arrived, joined, *, count):
    for i in range(count):
        put(joined, i, count, total(arrived, i, count))


def shape(rows):
    return jax.ShapeDtypeStruct((rows, R), F32)


def whole(array):
    zeros = (0,) * len(array.shape)
    return pl.BlockSpec(array.shape, lambda *_: zeros)


def operator(kernel, place, arrays, schur, outs, scratch):
    return pl.pallas_call(
        kernel,
        grid=(STEPS,),
        in_specs=[pl.BlockSpec(memory_space=pltpu.SMEM)]
        + [whole(a) for a in arrays]
        + [pl.BlockSpec((None, TILE, WINDOW), lambda i: (0, i, 0))],
        out_specs=[whole(o) for o in outs],
        out_shape=outs,
        scratch_shapes=scratch,
        compiler_params=pltpu.CompilerParams(
            dimension_semantics=("arbitrary",), vmem_limit_bytes=50 << 20
        ),
        cost_estimate=pl.CostEstimate(
            flops=8 * WINDOW * WINDOW * R, bytes_accessed=4 * WINDOW * WINDOW, transcendentals=0
        ),
    )(place, *arrays, schur)


def small_call(kernel, arrays, outs, place=None):
    head = [] if place is None else [place]
    return pl.pallas_call(
        kernel,
        in_specs=[pl.BlockSpec(memory_space=pltpu.SMEM)] * len(head)
        + [pl.BlockSpec(memory_space=pltpu.VMEM)] * len(arrays),
        out_specs=[pl.BlockSpec(memory_space=pltpu.VMEM)] * len(outs),
        out_shape=outs,
        compiler_params=pltpu.CompilerParams(vmem_limit_bytes=24 << 20),
        cost_estimate=pl.CostEstimate(
            flops=1 << 30, bytes_accessed=1 << 22, transcendentals=0
        ),
    )(*head, *arrays)


REMOTE = [(i, i + 1) for i in range(1, DEVICES - 1, 2)]
REMOTE = REMOTE + [(b, a) for a, b in REMOTE]


def swapped(to_partner, to_remote):
    remote = lax.ppermute(to_remote, GX_GY, REMOTE)
    partner = lax.ppermute(to_partner, "gy_2", [(0, 1), (1, 0)])
    return partner, remote


def halves_of(own, parity):
    at = SKIP * (1 - parity), SKIP * parity
    return [lax.dynamic_slice_in_dim(own, a, REACH, 0) for a in at]


def exchange(joined, count):
    sent = joined.reshape(DEVICES, 1, count * R)
    arrived = lax.all_to_all(sent, GX_GY, 0, 0, tiled=True)
    return arrived.reshape(DEVICES * count, R)


def summed(ends, place):
    own, *rest = ends
    arrived = swapped(*rest)
    own, *rest = small_call(
        sum_kernel, (own, *arrived), [shape(SLAB), shape(REACH), shape(REACH)], place
    )
    return own, *swapped(*rest)


def local(schur, offsets, right_side, basis, load):
    parity = lax.axis_index("gy_2").astype(jnp.int32)
    place = jnp.concatenate([offsets, parity[None]])
    ends = [shape(SLAB), shape(REACH), shape(REACH)]
    halves = pltpu.VMEM((WINDOW, 2 * R), BF16)
    ext = pltpu.VMEM((EXT, R), F32)
    rows = pltpu.VMEM((8, R), F32)
    square = pltpu.VMEM((R, R), F32)

    basis_sides = swapped(*halves_of(basis, parity))
    right_sides = swapped(*halves_of(right_side, parity))
    gram, coarse = contract_rows(basis, basis), contract_rows(basis, right_side)
    *image, joined = operator(
        first_kernel, place, (basis, *basis_sides, gram, coarse), schur,
        ends + [shape(3 * DEVICES)], [ext, halves, ext, rows, square],
    )
    arrived = exchange(joined, 3)
    image = summed(image, place)
    (joined,) = small_call(
        functools.partial(turn_kernel, count=3), (arrived,), [shape(3 * DEVICES)]
    )
    arrived = exchange(joined, 3)

    *w0, joined, r0, z_ext, inverse, first, amp, stiff = operator(
        start_kernel, place,
        (
            arrived, load, contract_rows(image[0], image[0]),
            right_side, *right_sides, basis, *basis_sides, *image,
        ),
        schur,
        ends + [shape(5 * DEVICES), EXTENDED, EXTENDED] + [MATRIX] * 4,
        [halves, ext, rows, square, square],
    )
    arrived = exchange(joined, 5)
    w0 = summed(w0, place)

    *w1, joined, r1, w0_ext, scalars = operator(
        middle_kernel, place, (arrived, r0, z_ext, *w0), schur,
        ends + [shape(5 * DEVICES), EXTENDED, EXTENDED, shape(8)], [halves, ext, rows, square],
    )
    arrived = exchange(joined, 5)
    w1 = summed(w1, place)

    joined, r2, numbers, matrices = operator(
        last_kernel, place,
        (arrived, scalars, r1, w0_ext, z_ext, *w1, inverse, stiff),
        schur,
        [shape(4 * DEVICES), shape(SLAB), shape(8), jax.ShapeDtypeStruct((4, R, R), F32)],
        [ext, halves, rows, ext],
    )
    arrived = exchange(joined, 4)
    base, d1, p2, small = small_call(
        direction_kernel,
        (numbers, matrices, inverse, stiff, first, basis, r0[OWN], r1[OWN], r2),
        [shape(SLAB)] * 3 + [jax.ShapeDtypeStruct((2, R, R), F32)],
    )
    return tuple(
        small_call(
            final_kernel,
            (arrived, numbers, matrices, small, inverse, amp, base, d1, p2),
            [shape(SLAB), MATRIX],
        )
    )


def solution(mesh):
    split = Mesh(mesh.devices.reshape(mesh.shape["gx"], 4, 4, 2), GX_GY)
    in_specs = (P(GX_GY, None, None), P(GX_GY), P(GX_GY, None), P(GX_GY, None), P())
    out_specs = (P(GX_GY, None), P())
    return jax.shard_map(local, mesh=split, in_specs=in_specs, out_specs=out_specs, check_vma=False)
```

```python
import functools

import jax
import jax.numpy as jnp
from jax import lax
from jax.experimental import pallas as pl
from jax.experimental.pallas import tpu as pltpu
from jax.sharding import Mesh
from jax.sharding import PartitionSpec as P

GX_GY = ("gx", "gy_0", "gy_1", "gy_2")
HIGHEST = lax.Precision.HIGHEST
F32 = jnp.float32
BF16 = jnp.bfloat16

SLAB = 1024
WINDOW = 2048
REACH = 768
SKIP = SLAB - REACH
HIGH = REACH + SLAB
EXT = SLAB + 2 * REACH
R = 128
DEVICES = 128
CHUNK = 512
STEPS = WINDOW // CHUNK
PIECES = 8
PIECE = WINDOW // PIECES
OWN = slice(REACH, HIGH)

MATRIX = jax.ShapeDtypeStruct((R, R), F32)
EXTENDED = jax.ShapeDtypeStruct((EXT, R), F32)


def full_dot(a, b):
    return jnp.dot(a, b, precision=HIGHEST, preferred_element_type=F32)


def contract_rows(a, b):
    return lax.dot_general(
        a, b, (((0,), (0,)), ((), ())), precision=HIGHEST, preferred_element_type=F32
    )


def split_bf16(x):
    high = x.astype(BF16)
    return high, (x - high.astype(F32)).astype(BF16)


def column_sum(a, b):
    return jnp.sum(a * b, axis=0, keepdims=True)


def part(arrived, index, count):
    return arrived[pl.ds(index, DEVICES, stride=count), :]


def total(arrived, index, count):
    return jnp.sum(part(arrived, index, count), axis=0, keepdims=True)


def put(joined, index, count, value):
    joined[pl.ds(index, DEVICES, stride=count), :] = jnp.broadcast_to(value, (DEVICES, R))


def sides(parity, scale):
    partner = pl.multiple_of(scale * (1 - parity), 8)
    remote = pl.multiple_of(scale * parity, 8)
    return pl.ds(partner, REACH), pl.ds(remote, REACH)


def assemble(ext, pieces, parity):
    own, partner, remote = pieces
    at_partner, at_remote = sides(parity, HIGH)
    ext[OWN, :] = own[...]
    ext[at_partner, :] = partner[...]
    ext[at_remote, :] = remote[...]


def invert(gram, inverse):
    row = lax.broadcasted_iota(jnp.int32, (R, R), 0)
    column = lax.broadcasted_iota(jnp.int32, (R, R), 1)
    identity = jnp.where(row == column, 1.0, 0.0).astype(F32)
    diagonal = gram * identity
    across = lax.rsqrt(jnp.sum(diagonal, axis=0, keepdims=True))
    along = lax.rsqrt(jnp.sum(diagonal, axis=1, keepdims=True))
    scaled = gram * across * along
    bound = jnp.max(jnp.sum(jnp.abs(scaled), axis=0, keepdims=True), axis=1, keepdims=True)
    inverse[...] = identity / bound

    def refine():
        current = inverse[...]
        rest = identity - full_dot(scaled, current)
        inverse[...] = current + full_dot(current, rest)
        return jnp.max(jnp.abs(rest))

    def body(carry):
        return carry[0] + 1, refine()

    lax.while_loop(lambda c: (c[0] < 60) & (c[1] > 1e-3), body, (jnp.int32(0), jnp.float32(1.0)))
    refine()
    inverse[...] = inverse[...] * across * along


def packed(x):
    return jnp.concatenate(split_bf16(x), axis=1)


def close_dot(x, m):
    high, low = split_bf16(m)
    upper = jnp.concatenate([high, low], axis=1)
    lower = jnp.concatenate([high, jnp.zeros_like(high)], axis=1)
    out = jnp.dot(packed(x), jnp.concatenate([upper, lower], axis=0), preferred_element_type=F32)
    return out[:, :R] + out[:, R:]


def close_contract(x, y):
    out = lax.dot_general(
        packed(x), packed(y), (((0,), (0,)), ((), ())), preferred_element_type=F32
    )
    return (out[:R, :R] + out[R:, R:]) + (out[:R, R:] + out[R:, :R])


def piece_of(schur, buffer, arrivals, index):
    rows = pl.ds(pl.multiple_of(index * PIECE, PIECE), PIECE)
    return pltpu.make_async_copy(schur.at[0, rows, :], buffer.at[rows, :], arrivals.at[index])


def fetch(schur, buffer, arrivals):
    for index in range(PIECES):
        piece_of(schur, buffer, arrivals, index).start()


def multiply(start, ext, schur, buffer, arrivals, halves, use):
    high, low = split_bf16(ext[pl.ds(start, WINDOW), :])
    halves[:, :R] = high
    halves[:, R:] = low

    def body(step, carry):
        for index in range(PIECES // STEPS):
            piece_of(schur, buffer, arrivals, step * (PIECES // STEPS) + index).wait()
        at = pl.multiple_of(step * CHUNK, CHUNK)
        high, low = split_bf16(buffer[pl.ds(at, CHUNK), :])
        both = jnp.dot(high, halves[...], preferred_element_type=F32)
        rest = jnp.dot(low, halves[:, :R], preferred_element_type=F32)
        use(pl.ds(start + at, CHUNK), both[:, :R] + both[:, R:] + rest)
        return carry

    lax.fori_loop(0, STEPS, body, 0)


def add_form(form, ext, rows, product):
    form[...] += jnp.sum((ext[rows, :] * product).reshape(CHUNK // 8, 8, R), axis=0)


def clear(form, cross, image):
    form[...] = jnp.zeros_like(form)
    cross[...] = jnp.zeros_like(cross)
    image[: EXT - WINDOW, :] = jnp.zeros((EXT - WINDOW, R), F32)
    image[WINDOW:, :] = jnp.zeros((EXT - WINDOW, R), F32)


def deliver(image, parity, own, partner, remote):
    at_partner, at_remote = sides(parity, HIGH)
    own[...] = image[OWN, :]
    partner[...] = image[at_partner, :]
    remote[...] = image[at_remote, :]


def first_kernel(
    place, own, partner, remote, gram, coarse, schur,
    out_own, out_partner, out_remote, joined,
    buffer, arrivals, halves, ext, image, form, cross,
):
    start, parity = place[0] - SKIP, place[1]
    fetch(schur, buffer, arrivals)
    assemble(ext, (own, partner, remote), parity)
    clear(form, cross, image)
    put(joined, 0, 3, gram[...])
    put(joined, 1, 3, coarse[...])

    def use(rows, product):
        cross[...] += close_contract(ext[rows, :], product)
        image[rows, :] = product

    multiply(start, ext, schur, buffer, arrivals, halves, use)
    deliver(image, parity, out_own, out_partner, out_remote)
    put(joined, 2, 3, cross[...])


def start_kernel(
    place, arrived, load, square,
    right_own, right_partner, right_remote,
    basis_own, basis_partner, basis_remote,
    image_own, image_partner, image_remote, schur,
    out_own, out_partner, out_remote, joined,
    residual, z_ext, new_own, inverse, first, amp, stiff,
    buffer, arrivals, halves, image, form, cross,
):
    start, parity = place[0] - SKIP, place[1]
    fetch(schur, buffer, arrivals)
    invert(part(arrived, 0, 3), inverse)
    stiff[...] = part(arrived, 2, 3)
    first[...] = full_dot(inverse[...], load[...])
    amp[...] = full_dot(inverse[...], part(arrived, 1, 3) - full_dot(stiff[...], first[...]))
    assemble(z_ext, (image_own, image_partner, image_remote), parity)
    assemble(image, (basis_own, basis_partner, basis_remote), parity)
    assemble(residual, (right_own, right_partner, right_remote), parity)
    residual[...] = (
        residual[...] - close_dot(z_ext[...], first[...]) - close_dot(image[...], amp[...])
    )
    clear(form, cross, image)
    own = residual[OWN, :]
    new_own[...] = own
    put(joined, 0, 5, column_sum(own, own))
    put(joined, 4, 5, square[...])
    put(joined, 2, 5, close_contract(image_own[...], own))

    def use(rows, product):
        add_form(form, residual, rows, product)
        cross[...] += close_contract(z_ext[rows, :], product)
        image[rows, :] = product

    multiply(start, residual, schur, buffer, arrivals, halves, use)
    deliver(image, parity, out_own, out_partner, out_remote)
    put(joined, 1, 5, jnp.sum(form[...], axis=0, keepdims=True))
    put(joined, 3, 5, cross[...])


def middle_kernel(
    place, arrived, last, z_ext, own, partner, remote, schur,
    out_own, out_partner, out_remote, joined, residual, w_ext, new_own, scalars,
    buffer, arrivals, halves, image, form, cross,
):
    start, parity = place[0] - SKIP, place[1]
    fetch(schur, buffer, arrivals)
    energy = total(arrived, 0, 5)
    length = energy / total(arrived, 1, 5)
    assemble(w_ext, (own, partner, remote), parity)
    residual[...] = last[...] - length * w_ext[...]
    clear(form, cross, image)
    mine = residual[OWN, :]
    new_own[...] = mine
    put(joined, 0, 5, column_sum(mine, mine))
    put(joined, 2, 5, total(arrived, 2, 5))
    put(joined, 3, 5, total(arrived, 3, 5))
    scalars[...] = jnp.zeros_like(scalars)
    scalars[0:1, :] = energy
    scalars[1:2, :] = length
    scalars[2:3, :] = total(arrived, 4, 5)

    def use(rows, product):
        add_form(form, residual, rows, product)
        cross[...] += close_contract(z_ext[rows, :], product)
        image[rows, :] = product

    multiply(start, residual, schur, buffer, arrivals, halves, use)
    deliver(image, parity, out_own, out_partner, out_remote)
    put(joined, 1, 5, jnp.sum(form[...], axis=0, keepdims=True))
    put(joined, 4, 5, cross[...])


def last_kernel(
    place, arrived, scalars, last, w_last, z_ext, own, partner, remote, inverse, stiff, schur,
    joined, new_own, numbers, matrices,
    buffer, arrivals, halves, residual, form, w_ext,
):
    start, parity = place[0] - SKIP, place[1]
    fetch(schur, buffer, arrivals)
    energy0, length0 = scalars[0:1, :], scalars[1:2, :]
    e0, f0 = part(arrived, 2, 5), part(arrived, 3, 5)
    c1 = -length0 * e0
    a1 = full_dot(inverse[...], c1)
    e1 = e0 - length0 * f0
    energy1 = total(arrived, 0, 5) - column_sum(c1, a1)
    stiff_a1 = full_dot(stiff[...], a1)
    ratio0 = energy1 / energy0
    curve1 = (
        total(arrived, 1, 5)
        - 2.0 * column_sum(a1, e1)
        + column_sum(a1, stiff_a1)
        - ratio0 * energy1 / length0
    )
    length1 = energy1 / curve1
    assemble(w_ext, (own, partner, remote), parity)
    residual[...] = last[...] - length1 * (
        w_ext[...] - close_dot(z_ext[...], a1) + ratio0 * w_last[...]
    )
    mine = residual[OWN, :]
    new_own[...] = mine
    put(joined, 0, 4, column_sum(mine, mine))
    put(joined, 2, 4, total(arrived, 4, 5))
    put(joined, 3, 4, scalars[2:3, :])
    numbers[...] = jnp.zeros_like(numbers)
    numbers[0:1, :] = length0
    numbers[1:2, :] = length1
    numbers[2:3, :] = ratio0
    numbers[3:4, :] = energy1
    d_coarse = e1 - stiff_a1 + ratio0 * e0
    matrices[0] = a1
    matrices[1] = c1 - length1 * d_coarse
    matrices[2] = d_coarse
    matrices[3] = e1 - length1 * ratio0 * f0
    form[...] = jnp.zeros_like(form)

    def use(rows, product):
        add_form(form, residual, rows, product)

    multiply(start, residual, schur, buffer, arrivals, halves, use)
    put(joined, 1, 4, jnp.sum(form[...], axis=0, keepdims=True))


def direction_kernel(
    numbers, matrices, inverse, stiff, first, basis, r0, r1, r2,
    base, d1, p2, small,
):
    length0, length1, ratio0 = numbers[0:1, :], numbers[1:2, :], numbers[2:3, :]
    a1 = matrices[0]
    a2 = full_dot(inverse[...], matrices[1])
    d1[...] = r1[...] - full_dot(basis[...], a1) + ratio0 * r0[...]
    p2[...] = r2[...] - full_dot(basis[...], a2)
    base[...] = full_dot(basis[...], first[...]) + length0 * r0[...] + length1 * d1[...]
    small[0] = a2
    small[1] = full_dot(stiff[...], a2)


def final_kernel(
    arrived, numbers, matrices, small, inverse, amp, base, d1, p2,
    multipliers, amplitudes,
):
    length1, energy1 = numbers[1:2, :], numbers[3:4, :]
    a2, stiff_a2 = small[0], small[1]
    f1, square = part(arrived, 2, 4), part(arrived, 3, 4)
    e2 = matrices[3] - length1 * (f1 - full_dot(square, matrices[0]))
    energy2 = total(arrived, 0, 4) - column_sum(matrices[1], a2)
    ratio1 = energy2 / energy1
    curve2 = (
        total(arrived, 1, 4)
        - 2.0 * column_sum(a2, e2)
        + column_sum(a2, stiff_a2)
        - ratio1 * energy2 / length1
    )
    length2 = energy2 / curve2
    multipliers[...] = base[...] + length2 * (p2[...] + ratio1 * d1[...])
    c3 = matrices[1] - length2 * (e2 - stiff_a2 + ratio1 * matrices[2])
    amplitudes[...] = amp[...] + full_dot(inverse[...], c3)


def sum_kernel(place, own, partner, remote, total_own, to_partner, to_remote):
    at_partner, at_remote = sides(place[1], SKIP)
    total_own[...] = own[...]
    total_own[at_partner, :] += partner[...]
    total_own[at_remote, :] += remote[...]
    to_partner[...] = total_own[at_partner, :]
    to_remote[...] = total_own[at_remote, :]


def turn_kernel(arrived, joined, *, count):
    for i in range(count):
        put(joined, i, count, total(arrived, i, count))


def shape(rows):
    return jax.ShapeDtypeStruct((rows, R), F32)


def operator(kernel, place, arrays, schur, outs, scratch):
    vmem = pl.BlockSpec(memory_space=pltpu.VMEM)
    return pl.pallas_call(
        kernel,
        in_specs=[pl.BlockSpec(memory_space=pltpu.SMEM)]
        + [vmem] * len(arrays)
        + [pl.BlockSpec(memory_space=pl.ANY)],
        out_specs=[vmem] * len(outs),
        out_shape=outs,
        scratch_shapes=[
            pltpu.VMEM((WINDOW, WINDOW), F32),
            pltpu.SemaphoreType.DMA((PIECES,)),
            pltpu.VMEM((WINDOW, 2 * R), BF16),
        ]
        + scratch,
        compiler_params=pltpu.CompilerParams(vmem_limit_bytes=50 << 20),
        cost_estimate=pl.CostEstimate(
            flops=8 * WINDOW * WINDOW * R, bytes_accessed=4 * WINDOW * WINDOW, transcendentals=0
        ),
    )(place, *arrays, schur)


def small_call(kernel, arrays, outs, place=None):
    head = [] if place is None else [place]
    return pl.pallas_call(
        kernel,
        in_specs=[pl.BlockSpec(memory_space=pltpu.SMEM)] * len(head)
        + [pl.BlockSpec(memory_space=pltpu.VMEM)] * len(arrays),
        out_specs=[pl.BlockSpec(memory_space=pltpu.VMEM)] * len(outs),
        out_shape=outs,
        compiler_params=pltpu.CompilerParams(vmem_limit_bytes=24 << 20),
        cost_estimate=pl.CostEstimate(
            flops=1 << 30, bytes_accessed=1 << 22, transcendentals=0
        ),
    )(*head, *arrays)


REMOTE = [(i, i + 1) for i in range(1, DEVICES - 1, 2)]
REMOTE = REMOTE + [(b, a) for a, b in REMOTE]


def swapped(to_partner, to_remote):
    remote = lax.ppermute(to_remote, GX_GY, REMOTE)
    partner = lax.ppermute(to_partner, "gy_2", [(0, 1), (1, 0)])
    return partner, remote


def halves_of(own, parity):
    at = SKIP * (1 - parity), SKIP * parity
    return [lax.dynamic_slice_in_dim(own, a, REACH, 0) for a in at]


def exchange(joined, count):
    sent = joined.reshape(DEVICES, 1, count * R)
    arrived = lax.all_to_all(sent, GX_GY, 0, 0, tiled=True)
    return arrived.reshape(DEVICES * count, R)


def summed(ends, place):
    own, *rest = ends
    arrived = swapped(*rest)
    own, *rest = small_call(
        sum_kernel, (own, *arrived), [shape(SLAB), shape(REACH), shape(REACH)], place
    )
    return own, *swapped(*rest)


def local(schur, offsets, right_side, basis, load):
    parity = lax.axis_index("gy_2").astype(jnp.int32)
    place = jnp.concatenate([offsets, parity[None]])
    ends = [shape(SLAB), shape(REACH), shape(REACH)]
    ext = pltpu.VMEM((EXT, R), F32)
    rows = pltpu.VMEM((8, R), F32)
    square = pltpu.VMEM((R, R), F32)

    basis_sides = swapped(*halves_of(basis, parity))
    right_sides = swapped(*halves_of(right_side, parity))
    gram, coarse = contract_rows(basis, basis), contract_rows(basis, right_side)
    *image, joined = operator(
        first_kernel, place, (basis, *basis_sides, gram, coarse), schur,
        ends + [shape(3 * DEVICES)], [ext, ext, rows, square],
    )
    arrived = exchange(joined, 3)
    image = summed(image, place)
    (joined,) = small_call(
        functools.partial(turn_kernel, count=3), (arrived,), [shape(3 * DEVICES)]
    )
    arrived = exchange(joined, 3)

    *w0, joined, r0_ext, z_ext, r0, inverse, first, amp, stiff = operator(
        start_kernel, place,
        (
            arrived, load, contract_rows(image[0], image[0]),
            right_side, *right_sides, basis, *basis_sides, *image,
        ),
        schur,
        ends + [shape(5 * DEVICES), EXTENDED, EXTENDED, shape(SLAB)] + [MATRIX] * 4,
        [ext, rows, square],
    )
    arrived = exchange(joined, 5)
    w0 = summed(w0, place)

    *w1, joined, r1_ext, w0_ext, r1, scalars = operator(
        middle_kernel, place, (arrived, r0_ext, z_ext, *w0), schur,
        ends + [shape(5 * DEVICES), EXTENDED, EXTENDED, shape(SLAB), shape(8)],
        [ext, rows, square],
    )
    arrived = exchange(joined, 5)
    w1 = summed(w1, place)

    joined, r2, numbers, matrices = operator(
        last_kernel, place,
        (arrived, scalars, r1_ext, w0_ext, z_ext, *w1, inverse, stiff),
        schur,
        [shape(4 * DEVICES), shape(SLAB), shape(8), jax.ShapeDtypeStruct((4, R, R), F32)],
        [ext, rows, ext],
    )
    arrived = exchange(joined, 4)
    base, d1, p2, small = small_call(
        direction_kernel,
        (numbers, matrices, inverse, stiff, first, basis, r0, r1, r2),
        [shape(SLAB)] * 3 + [jax.ShapeDtypeStruct((2, R, R), F32)],
    )
    return tuple(
        small_call(
            final_kernel,
            (arrived, numbers, matrices, small, inverse, amp, base, d1, p2),
            [shape(SLAB), MATRIX],
        )
    )


def solution(mesh):
    split = Mesh(mesh.devices.reshape(mesh.shape["gx"], 4, 4, 2), GX_GY)
    in_specs = (P(GX_GY, None, None), P(GX_GY), P(GX_GY, None), P(GX_GY, None), P())
    out_specs = (P(GX_GY, None), P())
    return jax.shard_map(local, mesh=split, in_specs=in_specs, out_specs=out_specs, check_vma=False)
```

```python
import functools

import jax
import jax.numpy as jnp
from jax import lax
from jax.experimental import pallas as pl
from jax.experimental.pallas import tpu as pltpu
from jax.sharding import Mesh
from jax.sharding import PartitionSpec as P

GX_GY = ("gx", "gy_0", "gy_1", "gy_2")
HIGHEST = lax.Precision.HIGHEST
F32 = jnp.float32
BF16 = jnp.bfloat16

SLAB = 1024
WINDOW = 2048
REACH = 768
SKIP = SLAB - REACH
HIGH = REACH + SLAB
EXT = SLAB + 2 * REACH
R = 128
DEVICES = 128
CHUNK = 512
STEPS = WINDOW // CHUNK
PIECES = 8
PIECE = WINDOW // PIECES
OWN = slice(REACH, HIGH)

MATRIX = jax.ShapeDtypeStruct((R, R), F32)
EXTENDED = jax.ShapeDtypeStruct((EXT, R), F32)


def full_dot(a, b):
    return jnp.dot(a, b, precision=HIGHEST, preferred_element_type=F32)


def contract_rows(a, b):
    return lax.dot_general(
        a, b, (((0,), (0,)), ((), ())), precision=HIGHEST, preferred_element_type=F32
    )


def split_bf16(x):
    high = x.astype(BF16)
    return high, (x - high.astype(F32)).astype(BF16)


def column_sum(a, b):
    return jnp.sum(a * b, axis=0, keepdims=True)


def part(arrived, index, count):
    return arrived[pl.ds(index, DEVICES, stride=count), :]


def total(arrived, index, count):
    return jnp.sum(part(arrived, index, count), axis=0, keepdims=True)


def put(joined, index, count, value):
    joined[pl.ds(index, DEVICES, stride=count), :] = jnp.broadcast_to(value, (DEVICES, R))


def sides(parity, scale):
    partner = pl.multiple_of(scale * (1 - parity), 8)
    remote = pl.multiple_of(scale * parity, 8)
    return pl.ds(partner, REACH), pl.ds(remote, REACH)


def assemble(ext, pieces, parity):
    own, partner, remote = pieces
    at_partner, at_remote = sides(parity, HIGH)
    ext[OWN, :] = own[...]
    ext[at_partner, :] = partner[...]
    ext[at_remote, :] = remote[...]


def invert(gram, inverse):
    row = lax.broadcasted_iota(jnp.int32, (R, R), 0)
    column = lax.broadcasted_iota(jnp.int32, (R, R), 1)
    identity = jnp.where(row == column, 1.0, 0.0).astype(F32)
    diagonal = gram * identity
    across = lax.rsqrt(jnp.sum(diagonal, axis=0, keepdims=True))
    along = lax.rsqrt(jnp.sum(diagonal, axis=1, keepdims=True))
    scaled = gram * across * along
    bound = jnp.max(jnp.sum(jnp.abs(scaled), axis=0, keepdims=True), axis=1, keepdims=True)
    inverse[...] = identity / bound

    def refine():
        current = inverse[...]
        rest = identity - full_dot(scaled, current)
        inverse[...] = current + full_dot(current, rest)
        return jnp.max(jnp.abs(rest))

    def body(carry):
        return carry[0] + 1, refine()

    lax.while_loop(lambda c: (c[0] < 60) & (c[1] > 1e-3), body, (jnp.int32(0), jnp.float32(1.0)))
    refine()
    inverse[...] = inverse[...] * across * along


def packed(x):
    return jnp.concatenate(split_bf16(x), axis=1)


def close_dot(x, m):
    high, low = split_bf16(m)
    upper = jnp.concatenate([high, low], axis=1)
    lower = jnp.concatenate([high, jnp.zeros_like(high)], axis=1)
    out = jnp.dot(packed(x), jnp.concatenate([upper, lower], axis=0), preferred_element_type=F32)
    return out[:, :R] + out[:, R:]


def close_contract(x, y):
    out = lax.dot_general(
        packed(x), packed(y), (((0,), (0,)), ((), ())), preferred_element_type=F32
    )
    return (out[:R, :R] + out[R:, R:]) + (out[:R, R:] + out[R:, :R])


def piece_of(schur, buffer, arrivals, index):
    rows = pl.ds(pl.multiple_of(index * PIECE, PIECE), PIECE)
    return pltpu.make_async_copy(schur.at[0, rows, :], buffer.at[rows, :], arrivals.at[index])


def fetch(schur, buffer, arrivals):
    for index in range(PIECES):
        piece_of(schur, buffer, arrivals, index).start()


def multiply(start, ext, schur, buffer, arrivals, halves, use):
    high, low = split_bf16(ext[pl.ds(start, WINDOW), :])
    halves[:, :R] = high
    halves[:, R:] = low

    def body(step, carry):
        for index in range(PIECES // STEPS):
            piece_of(schur, buffer, arrivals, step * (PIECES // STEPS) + index).wait()
        at = pl.multiple_of(step * CHUNK, CHUNK)
        high, low = split_bf16(buffer[pl.ds(at, CHUNK), :])
        both = jnp.dot(high, halves[...], preferred_element_type=F32)
        rest = jnp.dot(low, halves[:, :R], preferred_element_type=F32)
        use(pl.ds(start + at, CHUNK), both[:, :R] + both[:, R:] + rest)
        return carry

    lax.fori_loop(0, STEPS, body, 0)


def add_form(form, ext, rows, product):
    form[...] += jnp.sum((ext[rows, :] * product).reshape(CHUNK // 8, 8, R), axis=0)


def clear(form, cross, image):
    form[...] = jnp.zeros_like(form)
    cross[...] = jnp.zeros_like(cross)
    image[: EXT - WINDOW, :] = jnp.zeros((EXT - WINDOW, R), F32)
    image[WINDOW:, :] = jnp.zeros((EXT - WINDOW, R), F32)


def deliver(image, parity, own, partner, remote):
    at_partner, at_remote = sides(parity, HIGH)
    own[...] = image[OWN, :]
    partner[...] = image[at_partner, :]
    remote[...] = image[at_remote, :]


def first_kernel(
    place, own, partner, remote, right, schur,
    out_own, out_partner, out_remote, joined,
    buffer, arrivals, halves, ext, image, form, cross,
):
    start, parity = place[0] - SKIP, place[1]
    fetch(schur, buffer, arrivals)
    assemble(ext, (own, partner, remote), parity)
    clear(form, cross, image)
    put(joined, 0, 3, contract_rows(own[...], own[...]))
    put(joined, 1, 3, contract_rows(own[...], right[...]))

    def use(rows, product):
        cross[...] += close_contract(ext[rows, :], product)
        image[rows, :] = product

    multiply(start, ext, schur, buffer, arrivals, halves, use)
    deliver(image, parity, out_own, out_partner, out_remote)
    put(joined, 2, 3, cross[...])


def start_kernel(
    place, arrived, load,
    right_own, right_partner, right_remote,
    basis_own, basis_partner, basis_remote,
    image_own, image_partner, image_remote, schur,
    out_own, out_partner, out_remote, joined,
    out_residual, out_z, inverse, first, amp, stiff,
    buffer, arrivals, halves, residual, z_ext, image, form, cross, saved,
):
    start, parity = place[0] - SKIP, place[1]
    fetch(schur, buffer, arrivals)
    assemble(z_ext, (image_own, image_partner, image_remote), parity)
    save_z = pltpu.make_async_copy(z_ext, out_z, saved.at[0])
    save_z.start()
    put(joined, 4, 5, close_contract(image_own[...], image_own[...]))
    invert(part(arrived, 0, 3), inverse)
    stiff[...] = part(arrived, 2, 3)
    first[...] = full_dot(inverse[...], load[...])
    amp[...] = full_dot(inverse[...], part(arrived, 1, 3) - full_dot(stiff[...], first[...]))
    assemble(image, (basis_own, basis_partner, basis_remote), parity)
    assemble(residual, (right_own, right_partner, right_remote), parity)
    residual[...] = (
        residual[...] - close_dot(z_ext[...], first[...]) - close_dot(image[...], amp[...])
    )
    save = pltpu.make_async_copy(residual, out_residual, saved.at[1])
    save.start()
    clear(form, cross, image)
    own = residual[OWN, :]
    put(joined, 0, 5, column_sum(own, own))
    put(joined, 2, 5, close_contract(image_own[...], own))

    def use(rows, product):
        add_form(form, residual, rows, product)
        cross[...] += close_contract(z_ext[rows, :], product)
        image[rows, :] = product

    multiply(start, residual, schur, buffer, arrivals, halves, use)
    deliver(image, parity, out_own, out_partner, out_remote)
    put(joined, 1, 5, jnp.sum(form[...], axis=0, keepdims=True))
    put(joined, 3, 5, cross[...])
    save_z.wait()
    save.wait()


def middle_kernel(
    place, arrived, own, partner, remote, last, z_last, schur,
    out_own, out_partner, out_remote, joined, out_residual, out_w, scalars,
    buffer, arrivals, halves, residual, z_ext, w_ext, image, form, cross, saved,
):
    start, parity = place[0] - SKIP, place[1]
    load = pltpu.make_async_copy(last, residual, saved.at[0])
    load_z = pltpu.make_async_copy(z_last, z_ext, saved.at[1])
    load.start()
    load_z.start()
    fetch(schur, buffer, arrivals)
    energy = total(arrived, 0, 5)
    length = energy / total(arrived, 1, 5)
    assemble(w_ext, (own, partner, remote), parity)
    save_w = pltpu.make_async_copy(w_ext, out_w, saved.at[2])
    save_w.start()
    load.wait()
    residual[...] = residual[...] - length * w_ext[...]
    save = pltpu.make_async_copy(residual, out_residual, saved.at[3])
    save.start()
    clear(form, cross, image)
    mine = residual[OWN, :]
    put(joined, 0, 5, column_sum(mine, mine))
    put(joined, 2, 5, total(arrived, 2, 5))
    put(joined, 3, 5, total(arrived, 3, 5))
    scalars[...] = jnp.zeros_like(scalars)
    scalars[0:1, :] = energy
    scalars[1:2, :] = length
    scalars[2:3, :] = total(arrived, 4, 5)
    load_z.wait()

    def use(rows, product):
        add_form(form, residual, rows, product)
        cross[...] += close_contract(z_ext[rows, :], product)
        image[rows, :] = product

    multiply(start, residual, schur, buffer, arrivals, halves, use)
    deliver(image, parity, out_own, out_partner, out_remote)
    put(joined, 1, 5, jnp.sum(form[...], axis=0, keepdims=True))
    put(joined, 4, 5, cross[...])
    save_w.wait()
    save.wait()


def last_kernel(
    place, arrived, scalars, own, partner, remote, inverse, stiff, first, basis,
    last, w_last, z_last, schur,
    joined, base, d1, p2, numbers, matrices,
    buffer, arrivals, halves, residual, z_ext, w_ext, w_old, form, saved,
):
    start, parity = place[0] - SKIP, place[1]
    loads = [
        pltpu.make_async_copy(here, there, saved.at[index])
        for index, (here, there) in enumerate(
            ((z_last, z_ext), (last, residual), (w_last, w_old))
        )
    ]
    for load in loads:
        load.start()
    fetch(schur, buffer, arrivals)
    energy0, length0 = scalars[0:1, :], scalars[1:2, :]
    e0, f0 = part(arrived, 2, 5), part(arrived, 3, 5)
    c1 = -length0 * e0
    a1 = full_dot(inverse[...], c1)
    e1 = e0 - length0 * f0
    energy1 = total(arrived, 0, 5) - column_sum(c1, a1)
    stiff_a1 = full_dot(stiff[...], a1)
    ratio0 = energy1 / energy0
    curve1 = (
        total(arrived, 1, 5)
        - 2.0 * column_sum(a1, e1)
        + column_sum(a1, stiff_a1)
        - ratio0 * energy1 / length0
    )
    length1 = energy1 / curve1
    assemble(w_ext, (own, partner, remote), parity)
    for load in loads:
        load.wait()
    r1 = residual[OWN, :]
    r0 = r1 + length0 * w_old[OWN, :]
    d1[...] = r1 - close_dot(basis[...], a1) + ratio0 * r0
    base[...] = close_dot(basis[...], first[...]) + length0 * r0 + length1 * d1[...]
    residual[...] = residual[...] - length1 * (
        w_ext[...] - close_dot(z_ext[...], a1) + ratio0 * w_old[...]
    )
    mine = residual[OWN, :]
    put(joined, 0, 4, column_sum(mine, mine))
    put(joined, 2, 4, total(arrived, 4, 5))
    put(joined, 3, 4, scalars[2:3, :])
    numbers[...] = jnp.zeros_like(numbers)
    numbers[0:1, :] = length0
    numbers[1:2, :] = length1
    numbers[2:3, :] = ratio0
    numbers[3:4, :] = energy1
    d_coarse = e1 - stiff_a1 + ratio0 * e0
    c2 = c1 - length1 * d_coarse
    a2 = full_dot(inverse[...], c2)
    p2[...] = mine - close_dot(basis[...], a2)
    matrices[0] = a1
    matrices[1] = c2
    matrices[2] = d_coarse
    matrices[3] = e1 - length1 * ratio0 * f0
    matrices[4] = a2
    matrices[5] = full_dot(stiff[...], a2)
    form[...] = jnp.zeros_like(form)

    def use(rows, product):
        add_form(form, residual, rows, product)

    multiply(start, residual, schur, buffer, arrivals, halves, use)
    put(joined, 1, 4, jnp.sum(form[...], axis=0, keepdims=True))


def final_kernel(
    arrived, numbers, matrices, inverse, amp, base, d1, p2,
    multipliers, amplitudes,
):
    length1, energy1 = numbers[1:2, :], numbers[3:4, :]
    a2, stiff_a2 = matrices[4], matrices[5]
    f1, square = part(arrived, 2, 4), part(arrived, 3, 4)
    e2 = matrices[3] - length1 * (f1 - full_dot(square, matrices[0]))
    energy2 = total(arrived, 0, 4) - column_sum(matrices[1], a2)
    ratio1 = energy2 / energy1
    curve2 = (
        total(arrived, 1, 4)
        - 2.0 * column_sum(a2, e2)
        + column_sum(a2, stiff_a2)
        - ratio1 * energy2 / length1
    )
    length2 = energy2 / curve2
    multipliers[...] = base[...] + length2 * (p2[...] + ratio1 * d1[...])
    c3 = matrices[1] - length2 * (e2 - stiff_a2 + ratio1 * matrices[2])
    amplitudes[...] = amp[...] + full_dot(inverse[...], c3)


def sum_kernel(place, own, partner, remote, total_own, to_partner, to_remote):
    at_partner, at_remote = sides(place[1], SKIP)
    total_own[...] = own[...]
    total_own[at_partner, :] += partner[...]
    total_own[at_remote, :] += remote[...]
    to_partner[...] = total_own[at_partner, :]
    to_remote[...] = total_own[at_remote, :]


def turn_kernel(arrived, joined, *, count):
    for i in range(count):
        put(joined, i, count, total(arrived, i, count))


def shape(rows):
    return jax.ShapeDtypeStruct((rows, R), F32)


def operator(kernel, place, arrays, kept, schur, outs, scratch):
    vmem = pl.BlockSpec(memory_space=pltpu.VMEM)
    free = pl.BlockSpec(memory_space=pl.ANY)
    return pl.pallas_call(
        kernel,
        in_specs=[pl.BlockSpec(memory_space=pltpu.SMEM)]
        + [vmem] * len(arrays)
        + [free] * (len(kept) + 1),
        out_specs=[free if o is EXTENDED else vmem for o in outs],
        out_shape=outs,
        scratch_shapes=[
            pltpu.VMEM((WINDOW, WINDOW), F32),
            pltpu.SemaphoreType.DMA((PIECES,)),
            pltpu.VMEM((WINDOW, 2 * R), BF16),
        ]
        + scratch,
        compiler_params=pltpu.CompilerParams(vmem_limit_bytes=50 << 20),
        cost_estimate=pl.CostEstimate(
            flops=8 * WINDOW * WINDOW * R, bytes_accessed=4 * WINDOW * WINDOW, transcendentals=0
        ),
    )(place, *arrays, *kept, schur)


def small_call(kernel, arrays, outs, place=None):
    head = [] if place is None else [place]
    return pl.pallas_call(
        kernel,
        in_specs=[pl.BlockSpec(memory_space=pltpu.SMEM)] * len(head)
        + [pl.BlockSpec(memory_space=pltpu.VMEM)] * len(arrays),
        out_specs=[pl.BlockSpec(memory_space=pltpu.VMEM)] * len(outs),
        out_shape=outs,
        compiler_params=pltpu.CompilerParams(vmem_limit_bytes=24 << 20),
        cost_estimate=pl.CostEstimate(
            flops=1 << 30, bytes_accessed=1 << 22, transcendentals=0
        ),
    )(*head, *arrays)


REMOTE = [(i, i + 1) for i in range(1, DEVICES - 1, 2)]
REMOTE = REMOTE + [(b, a) for a, b in REMOTE]


def swapped(to_partner, to_remote):
    remote = lax.ppermute(to_remote, GX_GY, REMOTE)
    partner = lax.ppermute(to_partner, "gy_2", [(0, 1), (1, 0)])
    return partner, remote


def halves_of(own, parity):
    at = SKIP * (1 - parity), SKIP * parity
    return [lax.dynamic_slice_in_dim(own, a, REACH, 0) for a in at]


def exchange(joined, count):
    sent = joined.reshape(DEVICES, 1, count * R)
    arrived = lax.all_to_all(sent, GX_GY, 0, 0, tiled=True)
    return arrived.reshape(DEVICES * count, R)


def summed(ends, place):
    own, *rest = ends
    arrived = swapped(*rest)
    own, *rest = small_call(
        sum_kernel, (own, *arrived), [shape(SLAB), shape(REACH), shape(REACH)], place
    )
    return own, *swapped(*rest)


def local(schur, offsets, right_side, basis, load):
    parity = lax.axis_index("gy_2").astype(jnp.int32)
    place = jnp.concatenate([offsets, parity[None]])
    ends = [shape(SLAB), shape(REACH), shape(REACH)]
    ext = pltpu.VMEM((EXT, R), F32)
    rows = pltpu.VMEM((8, R), F32)
    square = pltpu.VMEM((R, R), F32)
    waits = pltpu.SemaphoreType.DMA((4,))

    basis_sides = swapped(*halves_of(basis, parity))
    right_sides = swapped(*halves_of(right_side, parity))
    *image, joined = operator(
        first_kernel, place, (basis, *basis_sides, right_side), (), schur,
        ends + [shape(3 * DEVICES)], [ext, ext, rows, square],
    )
    arrived = exchange(joined, 3)
    image = summed(image, place)
    (joined,) = small_call(
        functools.partial(turn_kernel, count=3), (arrived,), [shape(3 * DEVICES)]
    )
    arrived = exchange(joined, 3)

    *w0, joined, r0, z_ext, inverse, first, amp, stiff = operator(
        start_kernel, place,
        (arrived, load, right_side, *right_sides, basis, *basis_sides, *image), (), schur,
        ends + [shape(5 * DEVICES), EXTENDED, EXTENDED] + [MATRIX] * 4,
        [ext, ext, ext, rows, square, waits],
    )
    arrived = exchange(joined, 5)
    w0 = summed(w0, place)

    *w1, joined, r1, w0, scalars = operator(
        middle_kernel, place, (arrived, *w0), (r0, z_ext), schur,
        ends + [shape(5 * DEVICES), EXTENDED, EXTENDED, shape(8)],
        [ext, ext, ext, ext, rows, square, waits],
    )
    arrived = exchange(joined, 5)
    w1 = summed(w1, place)

    joined, base, d1, p2, numbers, matrices = operator(
        last_kernel, place,
        (arrived, scalars, *w1, inverse, stiff, first, basis), (r1, w0, z_ext), schur,
        [shape(4 * DEVICES)] + [shape(SLAB)] * 3
        + [shape(8), jax.ShapeDtypeStruct((6, R, R), F32)],
        [ext, ext, ext, ext, rows, waits],
    )
    arrived = exchange(joined, 4)
    return tuple(
        small_call(
            final_kernel,
            (arrived, numbers, matrices, inverse, amp, base, d1, p2),
            [shape(SLAB), MATRIX],
        )
    )


def solution(mesh):
    split = Mesh(mesh.devices.reshape(mesh.shape["gx"], 4, 4, 2), GX_GY)
    in_specs = (P(GX_GY, None, None), P(GX_GY), P(GX_GY, None), P(GX_GY, None), P())
    out_specs = (P(GX_GY, None), P())
    return jax.shard_map(local, mesh=split, in_specs=in_specs, out_specs=out_specs, check_vma=False)
```

```python
import functools

import jax
import jax.numpy as jnp
from jax import lax
from jax.experimental import pallas as pl
from jax.experimental.pallas import tpu as pltpu
from jax.sharding import Mesh
from jax.sharding import PartitionSpec as P

GX_GY = ("gx", "gy_0", "gy_1", "gy_2")
HIGHEST = lax.Precision.HIGHEST
F32 = jnp.float32
BF16 = jnp.bfloat16

SLAB = 1024
WINDOW = 2048
REACH = 768
SKIP = SLAB - REACH
HIGH = REACH + SLAB
EXT = SLAB + 2 * REACH
R = 128
DEVICES = 128
CHUNK = 512
STEPS = WINDOW // CHUNK
PIECES = 8
PIECE = WINDOW // PIECES
AHEAD = 4
OWN = slice(REACH, HIGH)

MATRIX = jax.ShapeDtypeStruct((R, R), F32)
EXTENDED = jax.ShapeDtypeStruct((EXT, R), F32)


def full_dot(a, b):
    return jnp.dot(a, b, precision=HIGHEST, preferred_element_type=F32)


def contract_rows(a, b):
    return lax.dot_general(
        a, b, (((0,), (0,)), ((), ())), precision=HIGHEST, preferred_element_type=F32
    )


def split_bf16(x):
    high = x.astype(BF16)
    return high, (x - high.astype(F32)).astype(BF16)


def column_sum(a, b):
    return jnp.sum(a * b, axis=0, keepdims=True)


def part(arrived, index, count):
    return arrived[pl.ds(index, DEVICES, stride=count), :]


def total(arrived, index, count):
    return jnp.sum(part(arrived, index, count), axis=0, keepdims=True)


def put(joined, index, count, value):
    joined[pl.ds(index, DEVICES, stride=count), :] = jnp.broadcast_to(value, (DEVICES, R))


def sides(parity, scale):
    partner = pl.multiple_of(scale * (1 - parity), 8)
    remote = pl.multiple_of(scale * parity, 8)
    return pl.ds(partner, REACH), pl.ds(remote, REACH)


def assemble(ext, pieces, parity):
    own, partner, remote = pieces
    at_partner, at_remote = sides(parity, HIGH)
    ext[OWN, :] = own[...]
    ext[at_partner, :] = partner[...]
    ext[at_remote, :] = remote[...]


def invert(gram, inverse):
    row = lax.broadcasted_iota(jnp.int32, (R, R), 0)
    column = lax.broadcasted_iota(jnp.int32, (R, R), 1)
    identity = jnp.where(row == column, 1.0, 0.0).astype(F32)
    diagonal = gram * identity
    across = lax.rsqrt(jnp.sum(diagonal, axis=0, keepdims=True))
    along = lax.rsqrt(jnp.sum(diagonal, axis=1, keepdims=True))
    scaled = gram * across * along
    bound = jnp.max(jnp.sum(jnp.abs(scaled), axis=0, keepdims=True), axis=1, keepdims=True)
    inverse[...] = identity / bound

    def refine():
        current = inverse[...]
        rest = identity - full_dot(scaled, current)
        inverse[...] = current + full_dot(current, rest)
        return jnp.max(jnp.abs(rest))

    def body(carry):
        return carry[0] + 1, refine()

    lax.while_loop(lambda c: (c[0] < 60) & (c[1] > 1e-3), body, (jnp.int32(0), jnp.float32(1.0)))
    refine()
    inverse[...] = inverse[...] * across * along


def packed(x):
    return jnp.concatenate(split_bf16(x), axis=1)


def close_dot(x, m):
    high, low = split_bf16(m)
    upper = jnp.concatenate([high, low], axis=1)
    lower = jnp.concatenate([high, jnp.zeros_like(high)], axis=1)
    out = jnp.dot(packed(x), jnp.concatenate([upper, lower], axis=0), preferred_element_type=F32)
    return out[:, :R] + out[:, R:]


def close_contract(x, y):
    out = lax.dot_general(
        packed(x), packed(y), (((0,), (0,)), ((), ())), preferred_element_type=F32
    )
    return (out[:R, :R] + out[R:, R:]) + (out[:R, R:] + out[R:, :R])


def piece_of(schur, buffer, arrivals, index):
    rows = pl.ds(pl.multiple_of(index * PIECE, PIECE), PIECE)
    return pltpu.make_async_copy(schur.at[0, rows, :], buffer.at[rows, :], arrivals.at[index])


def fetch(schur, buffer, arrivals, first, last):
    for index in range(first, last):
        piece_of(schur, buffer, arrivals, index).start()


def multiply(start, ext, schur, buffer, arrivals, halves, use):
    high, low = split_bf16(ext[pl.ds(start, WINDOW), :])
    halves[:, :R] = high
    halves[:, R:] = low

    def body(step, carry):
        for index in range(PIECES // STEPS):
            piece_of(schur, buffer, arrivals, step * (PIECES // STEPS) + index).wait()

        @pl.when(step < (PIECES - AHEAD) // (PIECES // STEPS))
        def _():
            for index in range(PIECES // STEPS):
                at = AHEAD + step * (PIECES // STEPS) + index
                piece_of(schur, buffer, arrivals, at).start()

        at = pl.multiple_of(step * CHUNK, CHUNK)
        high, low = split_bf16(buffer[pl.ds(at, CHUNK), :])
        both = jnp.dot(high, halves[...], preferred_element_type=F32)
        rest = jnp.dot(low, halves[:, :R], preferred_element_type=F32)
        use(pl.ds(start + at, CHUNK), both[:, :R] + both[:, R:] + rest)
        return carry

    lax.fori_loop(0, STEPS, body, 0)


def add_form(form, ext, rows, product):
    form[...] += jnp.sum((ext[rows, :] * product).reshape(CHUNK // 8, 8, R), axis=0)


def clear(form, cross, image):
    form[...] = jnp.zeros_like(form)
    cross[...] = jnp.zeros_like(cross)
    image[: EXT - WINDOW, :] = jnp.zeros((EXT - WINDOW, R), F32)
    image[WINDOW:, :] = jnp.zeros((EXT - WINDOW, R), F32)


def deliver(image, parity, own, partner, remote):
    at_partner, at_remote = sides(parity, HIGH)
    own[...] = image[OWN, :]
    partner[...] = image[at_partner, :]
    remote[...] = image[at_remote, :]


def first_kernel(
    place, own, partner, remote, right, schur,
    out_own, out_partner, out_remote, joined,
    buffer, arrivals, halves, ext, image, form, cross,
):
    start, parity = place[0] - SKIP, place[1]
    fetch(schur, buffer, arrivals, 0, AHEAD)
    assemble(ext, (own, partner, remote), parity)
    clear(form, cross, image)
    put(joined, 0, 3, contract_rows(own[...], own[...]))
    put(joined, 1, 3, contract_rows(own[...], right[...]))

    def use(rows, product):
        cross[...] += close_contract(ext[rows, :], product)
        image[rows, :] = product

    multiply(start, ext, schur, buffer, arrivals, halves, use)
    deliver(image, parity, out_own, out_partner, out_remote)
    put(joined, 2, 3, cross[...])


def start_kernel(
    place, arrived, load,
    right_own, right_partner, right_remote,
    basis_own, basis_partner, basis_remote,
    image_own, image_partner, image_remote, schur,
    out_own, out_partner, out_remote, joined,
    out_residual, out_z, inverse, first, amp, stiff,
    buffer, arrivals, halves, residual, z_ext, image, form, cross, saved,
):
    start, parity = place[0] - SKIP, place[1]
    fetch(schur, buffer, arrivals, 0, AHEAD)
    assemble(z_ext, (image_own, image_partner, image_remote), parity)
    save_z = pltpu.make_async_copy(z_ext, out_z, saved.at[0])
    save_z.start()
    put(joined, 4, 5, close_contract(image_own[...], image_own[...]))
    invert(part(arrived, 0, 3), inverse)
    stiff[...] = part(arrived, 2, 3)
    first[...] = full_dot(inverse[...], load[...])
    amp[...] = full_dot(inverse[...], part(arrived, 1, 3) - full_dot(stiff[...], first[...]))
    assemble(image, (basis_own, basis_partner, basis_remote), parity)
    assemble(residual, (right_own, right_partner, right_remote), parity)
    residual[...] = (
        residual[...] - close_dot(z_ext[...], first[...]) - close_dot(image[...], amp[...])
    )
    save = pltpu.make_async_copy(residual, out_residual, saved.at[1])
    save.start()
    clear(form, cross, image)
    own = residual[OWN, :]
    put(joined, 0, 5, column_sum(own, own))
    put(joined, 2, 5, close_contract(image_own[...], own))

    def use(rows, product):
        add_form(form, residual, rows, product)
        cross[...] += close_contract(z_ext[rows, :], product)
        image[rows, :] = product

    multiply(start, residual, schur, buffer, arrivals, halves, use)
    deliver(image, parity, out_own, out_partner, out_remote)
    put(joined, 1, 5, jnp.sum(form[...], axis=0, keepdims=True))
    put(joined, 3, 5, cross[...])
    save_z.wait()
    save.wait()


def middle_kernel(
    place, arrived, own, partner, remote, last, z_last, schur,
    out_own, out_partner, out_remote, joined, out_residual, out_w, scalars,
    buffer, arrivals, halves, residual, z_ext, w_ext, image, form, cross, saved,
):
    start, parity = place[0] - SKIP, place[1]
    load = pltpu.make_async_copy(last, residual, saved.at[0])
    load_z = pltpu.make_async_copy(z_last, z_ext, saved.at[1])
    load.start()
    load_z.start()
    fetch(schur, buffer, arrivals, 0, 2)
    energy = total(arrived, 0, 5)
    length = energy / total(arrived, 1, 5)
    assemble(w_ext, (own, partner, remote), parity)
    save_w = pltpu.make_async_copy(w_ext, out_w, saved.at[2])
    save_w.start()
    load.wait()
    fetch(schur, buffer, arrivals, 2, AHEAD)
    residual[...] = residual[...] - length * w_ext[...]
    save = pltpu.make_async_copy(residual, out_residual, saved.at[3])
    save.start()
    clear(form, cross, image)
    mine = residual[OWN, :]
    put(joined, 0, 5, column_sum(mine, mine))
    put(joined, 2, 5, total(arrived, 2, 5))
    put(joined, 3, 5, total(arrived, 3, 5))
    scalars[...] = jnp.zeros_like(scalars)
    scalars[0:1, :] = energy
    scalars[1:2, :] = length
    scalars[2:3, :] = total(arrived, 4, 5)
    load_z.wait()

    def use(rows, product):
        add_form(form, residual, rows, product)
        cross[...] += close_contract(z_ext[rows, :], product)
        image[rows, :] = product

    multiply(start, residual, schur, buffer, arrivals, halves, use)
    deliver(image, parity, out_own, out_partner, out_remote)
    put(joined, 1, 5, jnp.sum(form[...], axis=0, keepdims=True))
    put(joined, 4, 5, cross[...])
    save_w.wait()
    save.wait()


def last_kernel(
    place, arrived, scalars, own, partner, remote, inverse, stiff, first, basis,
    last, w_last, z_last, schur,
    joined, base, d1, p2, numbers, matrices,
    buffer, arrivals, halves, residual, z_ext, w_ext, w_old, form, saved,
):
    start, parity = place[0] - SKIP, place[1]
    loads = [
        pltpu.make_async_copy(here, there, saved.at[index])
        for index, (here, there) in enumerate(
            ((z_last, z_ext), (last, residual), (w_last, w_old))
        )
    ]
    for load in loads:
        load.start()
    fetch(schur, buffer, arrivals, 0, 1)
    energy0, length0 = scalars[0:1, :], scalars[1:2, :]
    e0, f0 = part(arrived, 2, 5), part(arrived, 3, 5)
    c1 = -length0 * e0
    a1 = full_dot(inverse[...], c1)
    e1 = e0 - length0 * f0
    energy1 = total(arrived, 0, 5) - column_sum(c1, a1)
    stiff_a1 = full_dot(stiff[...], a1)
    ratio0 = energy1 / energy0
    curve1 = (
        total(arrived, 1, 5)
        - 2.0 * column_sum(a1, e1)
        + column_sum(a1, stiff_a1)
        - ratio0 * energy1 / length0
    )
    length1 = energy1 / curve1
    assemble(w_ext, (own, partner, remote), parity)
    for load in loads:
        load.wait()
    fetch(schur, buffer, arrivals, 1, AHEAD)
    r1 = residual[OWN, :]
    r0 = r1 + length0 * w_old[OWN, :]
    d1[...] = r1 - close_dot(basis[...], a1) + ratio0 * r0
    base[...] = close_dot(basis[...], first[...]) + length0 * r0 + length1 * d1[...]
    residual[...] = residual[...] - length1 * (
        w_ext[...] - close_dot(z_ext[...], a1) + ratio0 * w_old[...]
    )
    mine = residual[OWN, :]
    put(joined, 0, 4, column_sum(mine, mine))
    put(joined, 2, 4, total(arrived, 4, 5))
    put(joined, 3, 4, scalars[2:3, :])
    numbers[...] = jnp.zeros_like(numbers)
    numbers[0:1, :] = length0
    numbers[1:2, :] = length1
    numbers[2:3, :] = ratio0
    numbers[3:4, :] = energy1
    d_coarse = e1 - stiff_a1 + ratio0 * e0
    c2 = c1 - length1 * d_coarse
    a2 = full_dot(inverse[...], c2)
    p2[...] = mine - close_dot(basis[...], a2)
    matrices[0] = a1
    matrices[1] = c2
    matrices[2] = d_coarse
    matrices[3] = e1 - length1 * ratio0 * f0
    matrices[4] = a2
    matrices[5] = full_dot(stiff[...], a2)
    form[...] = jnp.zeros_like(form)

    def use(rows, product):
        add_form(form, residual, rows, product)

    multiply(start, residual, schur, buffer, arrivals, halves, use)
    put(joined, 1, 4, jnp.sum(form[...], axis=0, keepdims=True))


def final_kernel(
    arrived, numbers, matrices, inverse, amp, base, d1, p2,
    multipliers, amplitudes,
):
    length1, energy1 = numbers[1:2, :], numbers[3:4, :]
    a2, stiff_a2 = matrices[4], matrices[5]
    f1, square = part(arrived, 2, 4), part(arrived, 3, 4)
    e2 = matrices[3] - length1 * (f1 - full_dot(square, matrices[0]))
    energy2 = total(arrived, 0, 4) - column_sum(matrices[1], a2)
    ratio1 = energy2 / energy1
    curve2 = (
        total(arrived, 1, 4)
        - 2.0 * column_sum(a2, e2)
        + column_sum(a2, stiff_a2)
        - ratio1 * energy2 / length1
    )
    length2 = energy2 / curve2
    multipliers[...] = base[...] + length2 * (p2[...] + ratio1 * d1[...])
    c3 = matrices[1] - length2 * (e2 - stiff_a2 + ratio1 * matrices[2])
    amplitudes[...] = amp[...] + full_dot(inverse[...], c3)


def sum_kernel(place, own, partner, remote, total_own, to_partner, to_remote):
    at_partner, at_remote = sides(place[1], SKIP)
    total_own[...] = own[...]
    total_own[at_partner, :] += partner[...]
    total_own[at_remote, :] += remote[...]
    to_partner[...] = total_own[at_partner, :]
    to_remote[...] = total_own[at_remote, :]


def turn_kernel(arrived, joined, *, count):
    for i in range(count):
        put(joined, i, count, total(arrived, i, count))


def shape(rows):
    return jax.ShapeDtypeStruct((rows, R), F32)


def operator(kernel, place, arrays, kept, schur, outs, scratch):
    vmem = pl.BlockSpec(memory_space=pltpu.VMEM)
    free = pl.BlockSpec(memory_space=pl.ANY)
    return pl.pallas_call(
        kernel,
        in_specs=[pl.BlockSpec(memory_space=pltpu.SMEM)]
        + [vmem] * len(arrays)
        + [free] * (len(kept) + 1),
        out_specs=[free if o is EXTENDED else vmem for o in outs],
        out_shape=outs,
        scratch_shapes=[
            pltpu.VMEM((WINDOW, WINDOW), F32),
            pltpu.SemaphoreType.DMA((PIECES,)),
            pltpu.VMEM((WINDOW, 2 * R), BF16),
        ]
        + scratch,
        compiler_params=pltpu.CompilerParams(vmem_limit_bytes=50 << 20),
        cost_estimate=pl.CostEstimate(
            flops=8 * WINDOW * WINDOW * R, bytes_accessed=4 * WINDOW * WINDOW, transcendentals=0
        ),
    )(place, *arrays, *kept, schur)


def small_call(kernel, arrays, outs, place=None):
    head = [] if place is None else [place]
    return pl.pallas_call(
        kernel,
        in_specs=[pl.BlockSpec(memory_space=pltpu.SMEM)] * len(head)
        + [pl.BlockSpec(memory_space=pltpu.VMEM)] * len(arrays),
        out_specs=[pl.BlockSpec(memory_space=pltpu.VMEM)] * len(outs),
        out_shape=outs,
        compiler_params=pltpu.CompilerParams(vmem_limit_bytes=24 << 20),
        cost_estimate=pl.CostEstimate(
            flops=1 << 30, bytes_accessed=1 << 22, transcendentals=0
        ),
    )(*head, *arrays)


REMOTE = [(i, i + 1) for i in range(1, DEVICES - 1, 2)]
REMOTE = REMOTE + [(b, a) for a, b in REMOTE]


def swapped(to_partner, to_remote):
    remote = lax.ppermute(to_remote, GX_GY, REMOTE)
    partner = lax.ppermute(to_partner, "gy_2", [(0, 1), (1, 0)])
    return partner, remote


def halves_of(own, parity):
    at = SKIP * (1 - parity), SKIP * parity
    return [lax.dynamic_slice_in_dim(own, a, REACH, 0) for a in at]


def exchange(joined, count):
    sent = joined.reshape(DEVICES, 1, count * R)
    arrived = lax.all_to_all(sent, GX_GY, 0, 0, tiled=True)
    return arrived.reshape(DEVICES * count, R)


def summed(ends, place):
    own, *rest = ends
    arrived = swapped(*rest)
    own, *rest = small_call(
        sum_kernel, (own, *arrived), [shape(SLAB), shape(REACH), shape(REACH)], place
    )
    return own, *swapped(*rest)


def local(schur, offsets, right_side, basis, load):
    parity = lax.axis_index("gy_2").astype(jnp.int32)
    place = jnp.concatenate([offsets, parity[None]])
    ends = [shape(SLAB), shape(REACH), shape(REACH)]
    ext = pltpu.VMEM((EXT, R), F32)
    rows = pltpu.VMEM((8, R), F32)
    square = pltpu.VMEM((R, R), F32)
    waits = pltpu.SemaphoreType.DMA((4,))

    basis_sides = swapped(*halves_of(basis, parity))
    right_sides = swapped(*halves_of(right_side, parity))
    *image, joined = operator(
        first_kernel, place, (basis, *basis_sides, right_side), (), schur,
        ends + [shape(3 * DEVICES)], [ext, ext, rows, square],
    )
    arrived = exchange(joined, 3)
    image = summed(image, place)
    (joined,) = small_call(
        functools.partial(turn_kernel, count=3), (arrived,), [shape(3 * DEVICES)]
    )
    arrived = exchange(joined, 3)

    *w0, joined, r0, z_ext, inverse, first, amp, stiff = operator(
        start_kernel, place,
        (arrived, load, right_side, *right_sides, basis, *basis_sides, *image), (), schur,
        ends + [shape(5 * DEVICES), EXTENDED, EXTENDED] + [MATRIX] * 4,
        [ext, ext, ext, rows, square, waits],
    )
    arrived = exchange(joined, 5)
    w0 = summed(w0, place)

    *w1, joined, r1, w0, scalars = operator(
        middle_kernel, place, (arrived, *w0), (r0, z_ext), schur,
        ends + [shape(5 * DEVICES), EXTENDED, EXTENDED, shape(8)],
        [ext, ext, ext, ext, rows, square, waits],
    )
    arrived = exchange(joined, 5)
    w1 = summed(w1, place)

    joined, base, d1, p2, numbers, matrices = operator(
        last_kernel, place,
        (arrived, scalars, *w1, inverse, stiff, first, basis), (r1, w0, z_ext), schur,
        [shape(4 * DEVICES)] + [shape(SLAB)] * 3
        + [shape(8), jax.ShapeDtypeStruct((6, R, R), F32)],
        [ext, ext, ext, ext, rows, waits],
    )
    arrived = exchange(joined, 4)
    return tuple(
        small_call(
            final_kernel,
            (arrived, numbers, matrices, inverse, amp, base, d1, p2),
            [shape(SLAB), MATRIX],
        )
    )


def solution(mesh):
    split = Mesh(mesh.devices.reshape(mesh.shape["gx"], 4, 4, 2), GX_GY)
    in_specs = (P(GX_GY, None, None), P(GX_GY), P(GX_GY, None), P(GX_GY, None), P())
    out_specs = (P(GX_GY, None), P())
    return jax.shard_map(local, mesh=split, in_specs=in_specs, out_specs=out_specs, check_vma=False)
```

```python
import functools

import jax
import jax.numpy as jnp
from jax import lax
from jax.experimental import pallas as pl
from jax.experimental.pallas import tpu as pltpu
from jax.sharding import Mesh
from jax.sharding import PartitionSpec as P

GX_GY = ("gx", "gy_0", "gy_1", "gy_2")
HIGHEST = lax.Precision.HIGHEST
F32 = jnp.float32
BF16 = jnp.bfloat16

SLAB = 1024
WINDOW = 2048
REACH = 768
SKIP = SLAB - REACH
HIGH = REACH + SLAB
EXT = SLAB + 2 * REACH
R = 128
DEVICES = 128
CHUNK = 512
STEPS = WINDOW // CHUNK
PIECES = 8
PIECE = WINDOW // PIECES
AHEAD = 4
OWN = slice(REACH, HIGH)

MATRIX = jax.ShapeDtypeStruct((R, R), F32)
EXTENDED = jax.ShapeDtypeStruct((EXT, R), F32)


def full_dot(a, b):
    return jnp.dot(a, b, precision=HIGHEST, preferred_element_type=F32)


def contract_rows(a, b):
    return lax.dot_general(
        a, b, (((0,), (0,)), ((), ())), precision=HIGHEST, preferred_element_type=F32
    )


def split_bf16(x):
    high = x.astype(BF16)
    return high, (x - high.astype(F32)).astype(BF16)


def column_sum(a, b):
    return jnp.sum(a * b, axis=0, keepdims=True)


def part(arrived, index, count):
    return arrived[pl.ds(index, DEVICES, stride=count), :]


def total(arrived, index, count):
    return jnp.sum(part(arrived, index, count), axis=0, keepdims=True)


def put(joined, index, count, value):
    joined[pl.ds(index, DEVICES, stride=count), :] = jnp.broadcast_to(value, (DEVICES, R))


def sides(parity, scale):
    partner = pl.multiple_of(scale * (1 - parity), 8)
    remote = pl.multiple_of(scale * parity, 8)
    return pl.ds(partner, REACH), pl.ds(remote, REACH)


def assemble(ext, pieces, parity):
    own, partner, remote = pieces
    at_partner, at_remote = sides(parity, HIGH)
    ext[OWN, :] = own[...]
    ext[at_partner, :] = partner[...]
    ext[at_remote, :] = remote[...]


def invert(gram, inverse):
    row = lax.broadcasted_iota(jnp.int32, (R, R), 0)
    column = lax.broadcasted_iota(jnp.int32, (R, R), 1)
    identity = jnp.where(row == column, 1.0, 0.0).astype(F32)
    diagonal = gram * identity
    across = lax.rsqrt(jnp.sum(diagonal, axis=0, keepdims=True))
    along = lax.rsqrt(jnp.sum(diagonal, axis=1, keepdims=True))
    scaled = gram * across * along
    bound = jnp.max(jnp.sum(jnp.abs(scaled), axis=0, keepdims=True), axis=1, keepdims=True)
    inverse[...] = identity / bound

    def refine():
        current = inverse[...]
        rest = identity - full_dot(scaled, current)
        inverse[...] = current + full_dot(current, rest)
        return jnp.max(jnp.abs(rest))

    def body(carry):
        return carry[0] + 1, refine()

    lax.while_loop(lambda c: (c[0] < 60) & (c[1] > 1e-3), body, (jnp.int32(0), jnp.float32(1.0)))
    refine()
    inverse[...] = inverse[...] * across * along


def packed(x):
    return jnp.concatenate(split_bf16(x), axis=1)


def close_dot(x, m):
    high, low = split_bf16(m)
    upper = jnp.concatenate([high, low], axis=1)
    lower = jnp.concatenate([high, jnp.zeros_like(high)], axis=1)
    out = jnp.dot(packed(x), jnp.concatenate([upper, lower], axis=0), preferred_element_type=F32)
    return out[:, :R] + out[:, R:]


def close_contract(x, y):
    out = lax.dot_general(
        packed(x), packed(y), (((0,), (0,)), ((), ())), preferred_element_type=F32
    )
    return (out[:R, :R] + out[R:, R:]) + (out[:R, R:] + out[R:, :R])


def piece_of(schur, buffer, arrivals, index):
    rows = pl.ds(pl.multiple_of(index * PIECE, PIECE), PIECE)
    return pltpu.make_async_copy(schur.at[0, rows, :], buffer.at[rows, :], arrivals.at[index])


def fetch(schur, buffer, arrivals, first, last):
    for index in range(first, last):
        piece_of(schur, buffer, arrivals, index).start()


def multiply(start, ext, schur, buffer, arrivals, halves, use):
    high, low = split_bf16(ext[pl.ds(start, WINDOW), :])
    halves[:, :R] = high
    halves[:, R:] = low

    def body(step, carry):
        for index in range(PIECES // STEPS):
            piece_of(schur, buffer, arrivals, step * (PIECES // STEPS) + index).wait()

        @pl.when(step < (PIECES - AHEAD) // (PIECES // STEPS))
        def _():
            for index in range(PIECES // STEPS):
                at = AHEAD + step * (PIECES // STEPS) + index
                piece_of(schur, buffer, arrivals, at).start()

        at = pl.multiple_of(step * CHUNK, CHUNK)
        high, low = split_bf16(buffer[pl.ds(at, CHUNK), :])
        both = jnp.dot(high, halves[...], preferred_element_type=F32)
        rest = jnp.dot(low, halves[:, :R], preferred_element_type=F32)
        use(pl.ds(start + at, CHUNK), both[:, :R] + both[:, R:] + rest)
        return carry

    lax.fori_loop(0, STEPS, body, 0)


def add_form(form, ext, rows, product):
    form[...] += jnp.sum((ext[rows, :] * product).reshape(CHUNK // 8, 8, R), axis=0)


def clear(form, cross, image):
    form[...] = jnp.zeros_like(form)
    cross[...] = jnp.zeros_like(cross)
    image[: EXT - WINDOW, :] = jnp.zeros((EXT - WINDOW, R), F32)
    image[WINDOW:, :] = jnp.zeros((EXT - WINDOW, R), F32)


def deliver(image, parity, own, partner, remote):
    at_partner, at_remote = sides(parity, HIGH)
    own[...] = image[OWN, :]
    partner[...] = image[at_partner, :]
    remote[...] = image[at_remote, :]


def gram_kernel(own, right, gram, coarse):
    gram[...] = contract_rows(own[...], own[...])
    coarse[...] = contract_rows(own[...], right[...])


def coarse_kernel(arrived, load, inverse, first, amp, stiff):
    invert(part(arrived, 0, 3), inverse)
    stiff[...] = part(arrived, 2, 3)
    first[...] = full_dot(inverse[...], load[...])
    amp[...] = full_dot(inverse[...], part(arrived, 1, 3) - full_dot(stiff[...], first[...]))


def plan_kernel(arrived, scalars, inverse, stiff, numbers, matrices):
    energy0, length0 = scalars[0:1, :], scalars[1:2, :]
    e0, f0 = part(arrived, 2, 5), part(arrived, 3, 5)
    c1 = -length0 * e0
    a1 = full_dot(inverse[...], c1)
    e1 = e0 - length0 * f0
    energy1 = total(arrived, 0, 5) - column_sum(c1, a1)
    stiff_a1 = full_dot(stiff[...], a1)
    ratio0 = energy1 / energy0
    curve1 = (
        total(arrived, 1, 5)
        - 2.0 * column_sum(a1, e1)
        + column_sum(a1, stiff_a1)
        - ratio0 * energy1 / length0
    )
    length1 = energy1 / curve1
    d_coarse = e1 - stiff_a1 + ratio0 * e0
    c2 = c1 - length1 * d_coarse
    a2 = full_dot(inverse[...], c2)
    numbers[...] = jnp.zeros_like(numbers)
    numbers[0:1, :] = length0
    numbers[1:2, :] = length1
    numbers[2:3, :] = ratio0
    numbers[3:4, :] = energy1
    numbers[4:5, :] = total(arrived, 4, 5)
    numbers[5:6, :] = scalars[2:3, :]
    matrices[0] = a1
    matrices[1] = c2
    matrices[2] = d_coarse
    matrices[3] = e1 - length1 * ratio0 * f0
    matrices[4] = a2
    matrices[5] = full_dot(stiff[...], a2)


def first_kernel(
    place, own, partner, remote, gram, coarse, schur,
    out_own, out_partner, out_remote, joined,
    buffer, arrivals, halves, ext, image, form, cross,
):
    start, parity = place[0] - SKIP, place[1]
    fetch(schur, buffer, arrivals, 0, 2)
    assemble(ext, (own, partner, remote), parity)
    clear(form, cross, image)
    put(joined, 0, 3, gram[...])
    put(joined, 1, 3, coarse[...])
    fetch(schur, buffer, arrivals, 2, AHEAD)

    def use(rows, product):
        cross[...] += close_contract(ext[rows, :], product)
        image[rows, :] = product

    multiply(start, ext, schur, buffer, arrivals, halves, use)
    deliver(image, parity, out_own, out_partner, out_remote)
    put(joined, 2, 3, cross[...])


def start_kernel(
    place, first, amp,
    right_own, right_partner, right_remote,
    basis_own, basis_partner, basis_remote,
    image_own, image_partner, image_remote, schur,
    out_own, out_partner, out_remote, joined,
    out_residual, out_z,
    buffer, arrivals, halves, residual, z_ext, image, form, cross, saved,
):
    start, parity = place[0] - SKIP, place[1]
    fetch(schur, buffer, arrivals, 0, AHEAD)
    assemble(z_ext, (image_own, image_partner, image_remote), parity)
    save_z = pltpu.make_async_copy(z_ext, out_z, saved.at[0])
    save_z.start()
    put(joined, 4, 5, close_contract(image_own[...], image_own[...]))
    assemble(image, (basis_own, basis_partner, basis_remote), parity)
    assemble(residual, (right_own, right_partner, right_remote), parity)
    residual[...] = (
        residual[...] - close_dot(z_ext[...], first[...]) - close_dot(image[...], amp[...])
    )
    save = pltpu.make_async_copy(residual, out_residual, saved.at[1])
    save.start()
    clear(form, cross, image)
    own = residual[OWN, :]
    put(joined, 0, 5, column_sum(own, own))
    put(joined, 2, 5, close_contract(image_own[...], own))

    def use(rows, product):
        add_form(form, residual, rows, product)
        cross[...] += close_contract(z_ext[rows, :], product)
        image[rows, :] = product

    multiply(start, residual, schur, buffer, arrivals, halves, use)
    deliver(image, parity, out_own, out_partner, out_remote)
    put(joined, 1, 5, jnp.sum(form[...], axis=0, keepdims=True))
    put(joined, 3, 5, cross[...])
    save_z.wait()
    save.wait()


def middle_kernel(
    place, arrived, own, partner, remote, last, z_last, schur,
    out_own, out_partner, out_remote, joined, out_residual, out_w, scalars,
    buffer, arrivals, halves, residual, z_ext, w_ext, image, form, cross, saved,
):
    start, parity = place[0] - SKIP, place[1]
    load = pltpu.make_async_copy(last, residual, saved.at[0])
    load_z = pltpu.make_async_copy(z_last, z_ext, saved.at[1])
    load.start()
    load_z.start()
    fetch(schur, buffer, arrivals, 0, 2)
    energy = total(arrived, 0, 5)
    length = energy / total(arrived, 1, 5)
    assemble(w_ext, (own, partner, remote), parity)
    save_w = pltpu.make_async_copy(w_ext, out_w, saved.at[2])
    save_w.start()
    load.wait()
    fetch(schur, buffer, arrivals, 2, AHEAD)
    residual[...] = residual[...] - length * w_ext[...]
    save = pltpu.make_async_copy(residual, out_residual, saved.at[3])
    save.start()
    clear(form, cross, image)
    mine = residual[OWN, :]
    put(joined, 0, 5, column_sum(mine, mine))
    put(joined, 2, 5, total(arrived, 2, 5))
    put(joined, 3, 5, total(arrived, 3, 5))
    scalars[...] = jnp.zeros_like(scalars)
    scalars[0:1, :] = energy
    scalars[1:2, :] = length
    scalars[2:3, :] = total(arrived, 4, 5)
    load_z.wait()

    def use(rows, product):
        add_form(form, residual, rows, product)
        cross[...] += close_contract(z_ext[rows, :], product)
        image[rows, :] = product

    multiply(start, residual, schur, buffer, arrivals, halves, use)
    deliver(image, parity, out_own, out_partner, out_remote)
    put(joined, 1, 5, jnp.sum(form[...], axis=0, keepdims=True))
    put(joined, 4, 5, cross[...])
    save_w.wait()
    save.wait()


def last_kernel(
    place, numbers, matrices, own, partner, remote, first, basis,
    last, w_last, z_last, schur,
    joined, base, d1, p2,
    buffer, arrivals, halves, residual, z_ext, w_ext, w_old, form, saved,
):
    start, parity = place[0] - SKIP, place[1]
    loads = [
        pltpu.make_async_copy(here, there, saved.at[index])
        for index, (here, there) in enumerate(
            ((z_last, z_ext), (last, residual), (w_last, w_old))
        )
    ]
    for load in loads:
        load.start()
    fetch(schur, buffer, arrivals, 0, 1)
    length0, length1, ratio0 = numbers[0:1, :], numbers[1:2, :], numbers[2:3, :]
    a1, a2 = matrices[0], matrices[4]
    form[...] = jnp.zeros_like(form)
    put(joined, 2, 4, numbers[4:5, :])
    put(joined, 3, 4, numbers[5:6, :])
    base[...] = close_dot(basis[...], first[...])
    d1[...] = close_dot(basis[...], a1)
    p2[...] = close_dot(basis[...], a2)
    assemble(w_ext, (own, partner, remote), parity)
    for load in loads:
        load.wait()
    fetch(schur, buffer, arrivals, 1, AHEAD)
    r1 = residual[OWN, :]
    r0 = r1 + length0 * w_old[OWN, :]
    d1[...] = r1 - d1[...] + ratio0 * r0
    base[...] = base[...] + length0 * r0 + length1 * d1[...]
    residual[...] = residual[...] - length1 * (
        w_ext[...] - close_dot(z_ext[...], a1) + ratio0 * w_old[...]
    )
    mine = residual[OWN, :]
    p2[...] = mine - p2[...]
    put(joined, 0, 4, column_sum(mine, mine))

    def use(rows, product):
        add_form(form, residual, rows, product)

    multiply(start, residual, schur, buffer, arrivals, halves, use)
    put(joined, 1, 4, jnp.sum(form[...], axis=0, keepdims=True))


def final_kernel(
    arrived, numbers, matrices, inverse, amp, base, d1, p2,
    multipliers, amplitudes,
):
    length1, energy1 = numbers[1:2, :], numbers[3:4, :]
    a2, stiff_a2 = matrices[4], matrices[5]
    f1, square = part(arrived, 2, 4), part(arrived, 3, 4)
    e2 = matrices[3] - length1 * (f1 - full_dot(square, matrices[0]))
    energy2 = total(arrived, 0, 4) - column_sum(matrices[1], a2)
    ratio1 = energy2 / energy1
    curve2 = (
        total(arrived, 1, 4)
        - 2.0 * column_sum(a2, e2)
        + column_sum(a2, stiff_a2)
        - ratio1 * energy2 / length1
    )
    length2 = energy2 / curve2
    multipliers[...] = base[...] + length2 * (p2[...] + ratio1 * d1[...])
    c3 = matrices[1] - length2 * (e2 - stiff_a2 + ratio1 * matrices[2])
    amplitudes[...] = amp[...] + full_dot(inverse[...], c3)


def sum_kernel(place, own, partner, remote, total_own, to_partner, to_remote):
    at_partner, at_remote = sides(place[1], SKIP)
    total_own[...] = own[...]
    total_own[at_partner, :] += partner[...]
    total_own[at_remote, :] += remote[...]
    to_partner[...] = total_own[at_partner, :]
    to_remote[...] = total_own[at_remote, :]


def turn_kernel(arrived, joined, *, count):
    for i in range(count):
        put(joined, i, count, total(arrived, i, count))


def shape(rows):
    return jax.ShapeDtypeStruct((rows, R), F32)


def operator(kernel, place, arrays, kept, schur, outs, scratch):
    vmem = pl.BlockSpec(memory_space=pltpu.VMEM)
    free = pl.BlockSpec(memory_space=pl.ANY)
    return pl.pallas_call(
        kernel,
        in_specs=[pl.BlockSpec(memory_space=pltpu.SMEM)]
        + [vmem] * len(arrays)
        + [free] * (len(kept) + 1),
        out_specs=[free if o is EXTENDED else vmem for o in outs],
        out_shape=outs,
        scratch_shapes=[
            pltpu.VMEM((WINDOW, WINDOW), F32),
            pltpu.SemaphoreType.DMA((PIECES,)),
            pltpu.VMEM((WINDOW, 2 * R), BF16),
        ]
        + scratch,
        compiler_params=pltpu.CompilerParams(vmem_limit_bytes=50 << 20),
        cost_estimate=pl.CostEstimate(
            flops=8 * WINDOW * WINDOW * R, bytes_accessed=4 * WINDOW * WINDOW, transcendentals=0
        ),
    )(place, *arrays, *kept, schur)


def small_call(kernel, arrays, outs, place=None):
    head = [] if place is None else [place]
    return pl.pallas_call(
        kernel,
        in_specs=[pl.BlockSpec(memory_space=pltpu.SMEM)] * len(head)
        + [pl.BlockSpec(memory_space=pltpu.VMEM)] * len(arrays),
        out_specs=[pl.BlockSpec(memory_space=pltpu.VMEM)] * len(outs),
        out_shape=outs,
        compiler_params=pltpu.CompilerParams(vmem_limit_bytes=24 << 20),
        cost_estimate=pl.CostEstimate(
            flops=1 << 30, bytes_accessed=1 << 22, transcendentals=0
        ),
    )(*head, *arrays)


REMOTE = [(i, i + 1) for i in range(1, DEVICES - 1, 2)]
REMOTE = REMOTE + [(b, a) for a, b in REMOTE]


def swapped(to_partner, to_remote):
    remote = lax.ppermute(to_remote, GX_GY, REMOTE)
    partner = lax.ppermute(to_partner, "gy_2", [(0, 1), (1, 0)])
    return partner, remote


def halves_of(own, parity):
    at = SKIP * (1 - parity), SKIP * parity
    return [lax.dynamic_slice_in_dim(own, a, REACH, 0) for a in at]


def exchange(joined, count):
    sent = joined.reshape(DEVICES, 1, count * R)
    arrived = lax.all_to_all(sent, GX_GY, 0, 0, tiled=True)
    return arrived.reshape(DEVICES * count, R)


def summed(ends, place):
    own, *rest = ends
    arrived = swapped(*rest)
    own, *rest = small_call(
        sum_kernel, (own, *arrived), [shape(SLAB), shape(REACH), shape(REACH)], place
    )
    return own, *swapped(*rest)


def local(schur, offsets, right_side, basis, load):
    parity = lax.axis_index("gy_2").astype(jnp.int32)
    place = jnp.concatenate([offsets, parity[None]])
    ends = [shape(SLAB), shape(REACH), shape(REACH)]
    ext = pltpu.VMEM((EXT, R), F32)
    rows = pltpu.VMEM((8, R), F32)
    square = pltpu.VMEM((R, R), F32)
    waits = pltpu.SemaphoreType.DMA((4,))

    basis_sides = swapped(*halves_of(basis, parity))
    right_sides = swapped(*halves_of(right_side, parity))
    gram, coarse = small_call(gram_kernel, (basis, right_side), [MATRIX] * 2)
    *image, joined = operator(
        first_kernel, place, (basis, *basis_sides, gram, coarse), (), schur,
        ends + [shape(3 * DEVICES)], [ext, ext, rows, square],
    )
    arrived = exchange(joined, 3)
    image = summed(image, place)
    (joined,) = small_call(
        functools.partial(turn_kernel, count=3), (arrived,), [shape(3 * DEVICES)]
    )
    arrived = exchange(joined, 3)

    inverse, first, amp, stiff = small_call(coarse_kernel, (arrived, load), [MATRIX] * 4)

    *w0, joined, r0, z_ext = operator(
        start_kernel, place,
        (first, amp, right_side, *right_sides, basis, *basis_sides, *image), (), schur,
        ends + [shape(5 * DEVICES), EXTENDED, EXTENDED],
        [ext, ext, ext, rows, square, waits],
    )
    arrived = exchange(joined, 5)
    w0 = summed(w0, place)

    *w1, joined, r1, w0, scalars = operator(
        middle_kernel, place, (arrived, *w0), (r0, z_ext), schur,
        ends + [shape(5 * DEVICES), EXTENDED, EXTENDED, shape(8)],
        [ext, ext, ext, ext, rows, square, waits],
    )
    arrived = exchange(joined, 5)
    w1 = summed(w1, place)

    numbers, matrices = small_call(
        plan_kernel, (arrived, scalars, inverse, stiff),
        [shape(8), jax.ShapeDtypeStruct((6, R, R), F32)],
    )

    joined, base, d1, p2 = operator(
        last_kernel, place,
        (numbers, matrices, *w1, first, basis), (r1, w0, z_ext), schur,
        [shape(4 * DEVICES)] + [shape(SLAB)] * 3,
        [ext, ext, ext, ext, rows, waits],
    )
    arrived = exchange(joined, 4)
    return tuple(
        small_call(
            final_kernel,
            (arrived, numbers, matrices, inverse, amp, base, d1, p2),
            [shape(SLAB), MATRIX],
        )
    )


def solution(mesh):
    split = Mesh(mesh.devices.reshape(mesh.shape["gx"], 4, 4, 2), GX_GY)
    in_specs = (P(GX_GY, None, None), P(GX_GY), P(GX_GY, None), P(GX_GY, None), P())
    out_specs = (P(GX_GY, None), P())
    return jax.shard_map(local, mesh=split, in_specs=in_specs, out_specs=out_specs, check_vma=False)
```
